8 devices in a mesh: dp: 1 (over z), tp: 8 (over y, x, core).
Axes of the slice: x: 2, y: 2, z: 1, core: 2. Of those that a mesh axis runs over, the one named last changes fastest.
Arguments:
- hidden: bfloat16 [1, 16, 2048], P('dp')
- norm_w: bfloat16 [2048], replicated
- embedding: bfloat16 [256000, 2048], P('tp')
- draft_ids: int32 [1, 16], P('dp')
Outputs:
- output 1: float32 [1, 16], P('dp')
- output 2: float32 [1, 16], P('dp')
All inputs are finite; a program needn't handle non-finite values.
Results may differ from the reference program's by a relative error of at most 0.001.
Values sent between devices are 32-bit elements.
A program may use at most 1 GiB of HBM per device.

```python
import jax
import jax.numpy as jnp
from jax import lax

BATCH = 1
DRAFT = 16
D = 2048
VOCAB = 256000
EPS = 1e-6
ROW_BLOCK = 2 ** 11
HOT_IDS = VOCAB // 16
ALIGN_SCALE = 6.0
NOISE_SCALE = 3.0


def draw_embedding(key_coef, key_noise, direction):
    num_blocks = VOCAB // ROW_BLOCK

    def one_block(block_idx):
        tok_coef = jax.random.normal(jax.random.fold_in(key_coef, block_idx), (ROW_BLOCK, 1), jnp.float32)
        noise_rows = jax.random.normal(jax.random.fold_in(key_noise, block_idx), (ROW_BLOCK, D), jnp.float32)
        block_rows = ALIGN_SCALE * tok_coef * direction / D + NOISE_SCALE * noise_rows * D ** -0.5
        return block_rows.astype(jnp.bfloat16)

    return lax.map(one_block, jnp.arange(num_blocks)).reshape(VOCAB, D)


def setup_inputs(seed: int = 0, part: int = 0) -> dict:
    base_key = jax.random.key(seed)
    key_dir, key_w, key_coef, key_noise, key_part = jax.random.split(base_key, 5)
    key_part = jax.random.fold_in(key_part, part)
    key_mix, key_hid, key_pick, key_low, key_any = jax.random.split(key_part, 5)
    direction = jax.random.normal(key_dir, (D,), jnp.float32)
    mix_coef = jax.random.uniform(key_mix, (BATCH, DRAFT, 1), jnp.float32, -0.9, 0.9)
    hid_noise = jax.random.normal(key_hid, (BATCH, DRAFT, D), jnp.float32)
    hidden = mix_coef * direction + jnp.sqrt(1.0 - mix_coef * mix_coef) * hid_noise
    norm_w = 0.5 * jax.random.normal(key_w, (D,), jnp.float32)
    embedding = draw_embedding(key_coef, key_noise, direction)
    pick_kind = jax.random.randint(key_pick, (BATCH, DRAFT), 0, 4)
    low_ids = jax.random.randint(key_low, (BATCH, DRAFT), 0, HOT_IDS)
    any_ids = jax.random.randint(key_any, (BATCH, DRAFT), 0, VOCAB)
    draft_ids = jnp.where(pick_kind < 3, low_ids, any_ids).astype(jnp.int32)
    draft_ids = draft_ids.at[0, 0].set(VOCAB - 1).at[0, 1].set(0)
    return {"hidden": hidden.astype(jnp.bfloat16), "norm_w": norm_w.astype(jnp.bfloat16), "embedding": embedding, "draft_ids": draft_ids}


def reference(hidden, norm_w, embedding, draft_ids):
    gain = 1.0 + norm_w.astype(jnp.float32)

    def one_seq(seq_args):
        seq_hidden, seq_ids = seq_args
        x_float = seq_hidden.astype(jnp.float32)
        mean_sq = jnp.mean(x_float * x_float, axis=-1, keepdims=True)
        normed = (x_float * lax.rsqrt(mean_sq + EPS) * gain).astype(jnp.bfloat16)
        logits = jnp.dot(normed, embedding.T, preferred_element_type=jnp.float32)
        row_max = jnp.max(logits, axis=-1, keepdims=True)
        exp_shift = jnp.exp(logits - row_max)
        exp_total = jnp.sum(exp_shift, axis=-1)
        weighted = jnp.sum(exp_shift * logits, axis=-1)
        log_norm = row_max[:, 0] + jnp.log(exp_total)
        picked = jnp.take_along_axis(logits, seq_ids[:, None], axis=-1)[:, 0]
        return picked - log_norm, log_norm - weighted / exp_total

    log_prob, entropy = lax.map(one_seq, (hidden, draft_ids))
    return log_prob, entropy
```

```python
import functools
import jax
import jax.numpy as jnp
from jax import lax
from jax.experimental import pallas as pl
from jax.experimental.pallas import tpu as pltpu
from jax.sharding import PartitionSpec as P

EPS = 1e-6
LANES = 128
BLOCK = 1280
DEPTH = 8
LOW = -3.0e38
MESH = pl.DeviceIdType.MESH


def head_kernel(n_dev, x_hbm, w_hbm, ids_hbm, e_hbm, lp_ref, en_ref,
                x_ref, w_ref, ids_ref, h_ref, buf, z_ref, stat, mine, got,
                small_sem, ring_sem, send_sem, recv_sem):
    rows = e_hbm.shape[0]
    pos = x_ref.shape[1]
    steps = rows // BLOCK
    me = lax.axis_index("tp")
    barrier = pltpu.get_barrier_semaphore()

    small = [pltpu.make_async_copy(s, d, small_sem.at[k])
             for k, (s, d) in enumerate(((x_hbm, x_ref), (w_hbm, w_ref), (ids_hbm, ids_ref)))]
    for c in small:
        c.start()

    def fetch(i):
        slot = lax.rem(i, DEPTH)
        return pltpu.make_async_copy(e_hbm.at[pl.ds(i * BLOCK, BLOCK), :], buf.at[slot], ring_sem.at[slot])

    for i in range(DEPTH - 1):
        fetch(i).start()
    for d in range(1, n_dev):
        pl.semaphore_signal(barrier, inc=1, device_id={"tp": lax.rem(me + d, n_dev)}, device_id_type=MESH)
    for c in small:
        c.wait()

    x = x_ref[0].astype(jnp.float32)
    r = lax.rsqrt(jnp.mean(x * x, axis=-1, keepdims=True) + EPS)
    gain = 1.0 + w_ref[...].astype(jnp.float32)
    for c in range(x.shape[1] // LANES):
        cols = slice(c * LANES, (c + 1) * LANES)
        h_ref[:, cols] = (x[:, cols] * r * gain[c:c + 1, :]).astype(jnp.bfloat16)

    sub = lax.broadcasted_iota(jnp.int32, (pos, pos), 0)
    lan = lax.broadcasted_iota(jnp.int32, (pos, pos), 1)
    eye = sub == lan
    ids_row = jnp.broadcast_to(ids_ref[...], (pos, pos)).astype(jnp.float32)
    ids_col = jnp.sum(jnp.where(eye, ids_row, 0.0), axis=1, keepdims=True).astype(jnp.int32)
    ids_rel = ids_col - me * rows - lax.broadcasted_iota(jnp.int32, (pos, LANES), 1)

    stat[0] = jnp.full((pos, LANES), LOW, jnp.float32)
    for k in range(1, 4):
        stat[k] = jnp.zeros((pos, LANES), jnp.float32)

    def logits(i):
        return lax.dot_general(h_ref[...], buf[lax.rem(i, DEPTH)], (((1,), (1,)), ((), ())),
                               preferred_element_type=jnp.float32)

    def fold(i):
        tiles = [z_ref[:, j * LANES:(j + 1) * LANES] for j in range(BLOCK // LANES)]
        m_old = stat[0]
        m_new = functools.reduce(jnp.maximum, tiles, m_old)
        scale = jnp.exp(m_old - m_new)
        s, a, p = stat[1] * scale, stat[2] * scale, stat[3]
        for j, t in enumerate(tiles):
            e = jnp.exp(t - m_new)
            s += e
            a += e * t
            p += jnp.where(ids_rel == i * BLOCK + j * LANES, t, 0.0)
        stat[0], stat[1], stat[2], stat[3] = m_new, s, a, p

    fetch(DEPTH - 1).start()
    fetch(0).wait()
    z_ref[...] = logits(0)

    def step(i, _):
        fetch(i).wait()
        nxt = i + DEPTH - 1

        @pl.when(nxt < steps)
        def _():
            fetch(nxt).start()

        z = logits(i)
        fold(i - 1)
        z_ref[...] = z
        return 0

    lax.fori_loop(1, steps, step, 0)
    fold(steps - 1)

    m_l, s_l, a_l, p_l = stat[0], stat[1], stat[2], stat[3]
    m_t, s_t, a_t, p_t = m_l.T, s_l.T, a_l.T, p_l.T
    m = jnp.max(m_t, axis=0, keepdims=True)
    wgt = jnp.exp(m_t - m)
    for k, v in enumerate((m, jnp.sum(s_t * wgt, axis=0, keepdims=True),
                           jnp.sum(a_t * wgt, axis=0, keepdims=True), jnp.sum(p_t, axis=0, keepdims=True))):
        mine[k:k + 1, :pos] = v
    got[me] = mine[...]
    pl.semaphore_wait(barrier, n_dev - 1)

    def send(d):
        peer = lax.rem(me + d, n_dev)
        return pltpu.make_async_remote_copy(
            src_ref=mine, dst_ref=got.at[me], send_sem=send_sem.at[d], recv_sem=recv_sem.at[me],
            device_id={"tp": peer}, device_id_type=MESH)

    def arrive(d):
        peer = lax.rem(me + d, n_dev)
        return pltpu.make_async_remote_copy(
            src_ref=mine, dst_ref=got.at[peer], send_sem=send_sem.at[d], recv_sem=recv_sem.at[peer],
            device_id={"tp": peer}, device_id_type=MESH)

    sends = [send(d) for d in range(1, n_dev)]
    for c in sends:
        c.start()
    for d in range(1, n_dev):
        arrive(d).wait_recv()
    ms = [got[d, 0:1, :pos] for d in range(n_dev)]
    top = functools.reduce(jnp.maximum, ms)
    ws = [jnp.exp(v - top) for v in ms]
    total = sum(got[d, 1:2, :pos] * ws[d] for d in range(n_dev))
    weighted = sum(got[d, 2:3, :pos] * ws[d] for d in range(n_dev))
    picked = sum(got[d, 3:4, :pos] for d in range(n_dev))
    log_norm = top + jnp.log(total)
    lp_ref[...] = picked - log_norm
    en_ref[...] = log_norm - weighted / total
    for c in sends:
        c.wait_send()


def solution(mesh):
    n_dev = mesh.shape["tp"]

    def local_part(hidden, norm_w, embedding, draft_ids):
        _, pos, width = hidden.shape
        hbm = pl.BlockSpec(memory_space=pltpu.HBM)
        vmem = pl.BlockSpec(memory_space=pltpu.VMEM)
        return pl.pallas_call(
            functools.partial(head_kernel, n_dev),
            out_shape=[jax.ShapeDtypeStruct((1, pos), jnp.float32)] * 2,
            in_specs=[hbm] * 4,
            out_specs=[vmem] * 2,
            scratch_shapes=[
                pltpu.VMEM((1, pos, width), jnp.bfloat16),
                pltpu.VMEM((width // LANES, LANES), jnp.bfloat16),
                pltpu.VMEM((1, pos), jnp.int32),
                pltpu.VMEM((pos, width), jnp.bfloat16),
                pltpu.VMEM((DEPTH, BLOCK, width), jnp.bfloat16),
                pltpu.VMEM((pos, BLOCK), jnp.float32),
                pltpu.VMEM((4, pos, LANES), jnp.float32),
                pltpu.VMEM((8, LANES), jnp.float32),
                pltpu.VMEM((n_dev, 8, LANES), jnp.float32),
                pltpu.SemaphoreType.DMA((3,)),
                pltpu.SemaphoreType.DMA((DEPTH,)),
                pltpu.SemaphoreType.DMA((n_dev,)),
                pltpu.SemaphoreType.DMA((n_dev,)),
            ],
            compiler_params=pltpu.CompilerParams(
                collective_id=0, has_side_effects=True, vmem_limit_bytes=60 * 2**20),
            cost_estimate=pl.CostEstimate(flops=2 * pos * embedding.size, bytes_accessed=2 * embedding.size,
                                          transcendentals=pos * embedding.shape[0]),
            name="head",
        )(hidden, norm_w.reshape(width // LANES, LANES), draft_ids, embedding)

    return jax.shard_map(local_part, mesh=mesh,
                         in_specs=(P("dp", None, None), P(None), P("tp", None), P("dp", None)),
                         out_specs=(P("dp", None), P("dp", None)), check_vma=False)
```

```python
import functools
import jax
import jax.numpy as jnp
from jax import lax
from jax.experimental import pallas as pl
from jax.experimental.pallas import tpu as pltpu
from jax.sharding import PartitionSpec as P

EPS = 1e-6
LANES = 128
BLOCK = 1280
DEPTH = 8
LOW = -3.0e38
MESH = pl.DeviceIdType.MESH


def head_kernel(n_dev, x_hbm, w_hbm, ids_hbm, e_hbm, out_ref,
                x_ref, w_ref, ids_ref, h_ref, buf, z_ref, stat, mine, got,
                small_sem, ring_sem, send_sem, recv_sem):
    rows = e_hbm.shape[0]
    pos = x_ref.shape[1]
    steps = rows // BLOCK
    me = lax.axis_index("tp")
    barrier = pltpu.get_barrier_semaphore()

    small = [pltpu.make_async_copy(s, d, small_sem.at[k])
             for k, (s, d) in enumerate(((x_hbm, x_ref), (w_hbm, w_ref), (ids_hbm, ids_ref)))]
    for c in small:
        c.start()

    def fetch(i):
        slot = lax.rem(i, DEPTH)
        return pltpu.make_async_copy(e_hbm.at[pl.ds(i * BLOCK, BLOCK), :], buf.at[slot], ring_sem.at[slot])

    for i in range(DEPTH - 1):
        fetch(i).start()
    for d in range(1, n_dev):
        pl.semaphore_signal(barrier, inc=1, device_id={"tp": lax.rem(me + d, n_dev)}, device_id_type=MESH)
    for c in small:
        c.wait()

    x = x_ref[0].astype(jnp.float32)
    r = lax.rsqrt(jnp.mean(x * x, axis=-1, keepdims=True) + EPS)
    gain = 1.0 + w_ref[...].astype(jnp.float32)
    for c in range(x.shape[1] // LANES):
        cols = slice(c * LANES, (c + 1) * LANES)
        h_ref[:, cols] = (x[:, cols] * r * gain[c:c + 1, :]).astype(jnp.bfloat16)

    sub = lax.broadcasted_iota(jnp.int32, (pos, pos), 0)
    lan = lax.broadcasted_iota(jnp.int32, (pos, pos), 1)
    eye = sub == lan
    ids_row = jnp.broadcast_to(ids_ref[...], (pos, pos)).astype(jnp.float32)
    ids_col = jnp.sum(jnp.where(eye, ids_row, 0.0), axis=1, keepdims=True).astype(jnp.int32)
    ids_rel = ids_col - me * rows - lax.broadcasted_iota(jnp.int32, (pos, LANES), 1)

    stat[0] = jnp.full((pos, LANES), LOW, jnp.float32)
    for k in range(1, 4):
        stat[k] = jnp.zeros((pos, LANES), jnp.float32)

    def logits(i):
        return lax.dot_general(h_ref[...], buf[lax.rem(i, DEPTH)], (((1,), (1,)), ((), ())),
                               preferred_element_type=jnp.float32)

    def fold(i):
        tiles = [z_ref[:, j * LANES:(j + 1) * LANES] for j in range(BLOCK // LANES)]
        m_old = stat[0]
        m_new = functools.reduce(jnp.maximum, tiles, m_old)
        scale = jnp.exp(m_old - m_new)
        s, a, p = stat[1] * scale, stat[2] * scale, stat[3]
        for j, t in enumerate(tiles):
            e = jnp.exp(t - m_new)
            s += e
            a += e * t
            p += jnp.where(ids_rel == i * BLOCK + j * LANES, t, 0.0)
        stat[0], stat[1], stat[2], stat[3] = m_new, s, a, p

    fetch(DEPTH - 1).start()
    fetch(0).wait()
    z_ref[...] = logits(0)

    def step(i, _):
        fetch(i).wait()
        nxt = i + DEPTH - 1

        @pl.when(nxt < steps)
        def _():
            fetch(nxt).start()

        z = logits(i)
        fold(i - 1)
        z_ref[...] = z
        return 0

    lax.fori_loop(1, steps, step, 0)
    fold(steps - 1)

    m_l, s_l, a_l, p_l = stat[0], stat[1], stat[2], stat[3]
    m_t, s_t, a_t, p_t = m_l.T, s_l.T, a_l.T, p_l.T
    m = jnp.max(m_t, axis=0, keepdims=True)
    wgt = jnp.exp(m_t - m)
    for k, v in enumerate((m, jnp.sum(s_t * wgt, axis=0, keepdims=True),
                           jnp.sum(a_t * wgt, axis=0, keepdims=True), jnp.sum(p_t, axis=0, keepdims=True))):
        mine[k:k + 1, :pos] = v
    got[me] = mine[...]
    pl.semaphore_wait(barrier, n_dev - 1)

    def send(d):
        peer = lax.rem(me + d, n_dev)
        return pltpu.make_async_remote_copy(
            src_ref=mine, dst_ref=got.at[me], send_sem=send_sem.at[d], recv_sem=recv_sem.at[me],
            device_id={"tp": peer}, device_id_type=MESH)

    def arrive(d):
        peer = lax.rem(me + d, n_dev)
        return pltpu.make_async_remote_copy(
            src_ref=mine, dst_ref=got.at[peer], send_sem=send_sem.at[d], recv_sem=recv_sem.at[peer],
            device_id={"tp": peer}, device_id_type=MESH)

    sends = [send(d) for d in range(1, n_dev)]
    for c in sends:
        c.start()
    for d in range(1, n_dev):
        arrive(d).wait_recv()
    ms = [got[d, 0:1, :pos] for d in range(n_dev)]
    top = functools.reduce(jnp.maximum, ms)
    ws = [jnp.exp(v - top) for v in ms]
    total = sum(got[d, 1:2, :pos] * ws[d] for d in range(n_dev))
    weighted = sum(got[d, 2:3, :pos] * ws[d] for d in range(n_dev))
    picked = sum(got[d, 3:4, :pos] for d in range(n_dev))
    for k, v in enumerate((top, total, weighted, picked)):
        out_ref[k:k + 1, :pos] = v
    for c in sends:
        c.wait_send()


def solution(mesh):
    n_dev = mesh.shape["tp"]

    def local_part(hidden, norm_w, embedding, draft_ids):
        _, pos, width = hidden.shape
        hbm = pl.BlockSpec(memory_space=pltpu.HBM)
        vmem = pl.BlockSpec(memory_space=pltpu.VMEM)
        out = pl.pallas_call(
            functools.partial(head_kernel, n_dev),
            out_shape=pltpu.VMEM((8, LANES), jnp.float32),
            in_specs=[hbm] * 4,
            out_specs=vmem,
            scratch_shapes=[
                pltpu.VMEM((1, pos, width), jnp.bfloat16),
                pltpu.VMEM((width // LANES, LANES), jnp.bfloat16),
                pltpu.VMEM((1, pos), jnp.int32),
                pltpu.VMEM((pos, width), jnp.bfloat16),
                pltpu.VMEM((DEPTH, BLOCK, width), jnp.bfloat16),
                pltpu.VMEM((pos, BLOCK), jnp.float32),
                pltpu.VMEM((4, pos, LANES), jnp.float32),
                pltpu.VMEM((8, LANES), jnp.float32),
                pltpu.VMEM((n_dev, 8, LANES), jnp.float32),
                pltpu.SemaphoreType.DMA((3,)),
                pltpu.SemaphoreType.DMA((DEPTH,)),
                pltpu.SemaphoreType.DMA((n_dev,)),
                pltpu.SemaphoreType.DMA((n_dev,)),
            ],
            compiler_params=pltpu.CompilerParams(
                collective_id=0, has_side_effects=True, vmem_limit_bytes=60 * 2**20),
            cost_estimate=pl.CostEstimate(flops=2 * pos * embedding.size, bytes_accessed=2 * embedding.size,
                                          transcendentals=pos * embedding.shape[0]),
            name="head",
        )(hidden, norm_w.reshape(width // LANES, LANES), draft_ids, embedding)
        top, total, weighted, picked = (out[k:k + 1, :pos] for k in range(4))
        log_norm = top + jnp.log(total)
        return picked - log_norm, log_norm - weighted / total

    return jax.shard_map(local_part, mesh=mesh,
                         in_specs=(P("dp", None, None), P(None), P("tp", None), P("dp", None)),
                         out_specs=(P("dp", None), P("dp", None)), check_vma=False)
```

```python
import functools
import jax
import jax.numpy as jnp
from jax import lax
from jax.experimental import pallas as pl
from jax.experimental.pallas import tpu as pltpu
from jax.sharding import PartitionSpec as P

EPS = 1e-6
LANES = 128
BLOCK = 1280
DEPTH = 8
LOW = -3.0e38
MESH = pl.DeviceIdType.MESH


def stream_kernel(x_hbm, w_hbm, ids_hbm, e_hbm, out_ref,
                  x_ref, w_ref, ids_ref, h_ref, buf, z_ref, stat, small_sem, ring_sem):
    rows = e_hbm.shape[0]
    pos = x_ref.shape[1]
    steps = rows // BLOCK

    small = [pltpu.make_async_copy(s, d, small_sem.at[k])
             for k, (s, d) in enumerate(((x_hbm, x_ref), (w_hbm, w_ref), (ids_hbm, ids_ref)))]
    for c in small:
        c.start(priority=0)

    def fetch(i):
        slot = lax.rem(i, DEPTH)
        return pltpu.make_async_copy(e_hbm.at[pl.ds(i * BLOCK, BLOCK), :], buf.at[slot], ring_sem.at[slot])

    for i in range(DEPTH):
        fetch(i).start(priority=1)
    for c in small:
        c.wait()

    x = x_ref[0].astype(jnp.float32)
    r = lax.rsqrt(jnp.mean(x * x, axis=-1, keepdims=True) + EPS)
    gain = 1.0 + w_ref[...].astype(jnp.float32)
    for c in range(x.shape[1] // LANES):
        cols = slice(c * LANES, (c + 1) * LANES)
        h_ref[:, cols] = (x[:, cols] * r * gain[c:c + 1, :]).astype(jnp.bfloat16)

    sub = lax.broadcasted_iota(jnp.int32, (pos, pos), 0)
    lan = lax.broadcasted_iota(jnp.int32, (pos, pos), 1)
    ids_row = jnp.broadcast_to(ids_ref[...], (pos, pos)).astype(jnp.float32)
    ids_col = jnp.sum(jnp.where(sub == lan, ids_row, 0.0), axis=1, keepdims=True).astype(jnp.int32)
    ids_rel = ids_col - lax.axis_index("tp") * rows - lax.broadcasted_iota(jnp.int32, (pos, LANES), 1)

    stat[0] = jnp.full((pos, LANES), LOW, jnp.float32)
    for k in range(1, 4):
        stat[k] = jnp.zeros((pos, LANES), jnp.float32)

    def logits(i):
        return lax.dot_general(h_ref[...], buf[lax.rem(i, DEPTH)], (((1,), (1,)), ((), ())),
                               preferred_element_type=jnp.float32)

    def fold(i):
        tiles = [z_ref[:, j * LANES:(j + 1) * LANES] for j in range(BLOCK // LANES)]
        m_old = stat[0]
        m_new = functools.reduce(jnp.maximum, tiles, m_old)
        scale = jnp.exp(m_old - m_new)
        s, a, p = stat[1] * scale, stat[2] * scale, stat[3]
        for j, t in enumerate(tiles):
            e = jnp.exp(t - m_new)
            s += e
            a += e * t
            p += jnp.where(ids_rel == i * BLOCK + j * LANES, t, 0.0)
        stat[0], stat[1], stat[2], stat[3] = m_new, s, a, p

    fetch(0).wait()
    z_ref[...] = logits(0)

    def step(i, _):
        fetch(i).wait()
        nxt = i + DEPTH - 1

        @pl.when(nxt < steps)
        def _():
            fetch(nxt).start(priority=1)

        z = logits(i)
        fold(i - 1)
        z_ref[...] = z
        return 0

    lax.fori_loop(1, steps, step, 0)
    fold(steps - 1)

    m_t, s_t, a_t, p_t = stat[0].T, stat[1].T, stat[2].T, stat[3].T
    m = jnp.max(m_t, axis=0, keepdims=True)
    wgt = jnp.exp(m_t - m)
    for k, v in enumerate((m, jnp.sum(s_t * wgt, axis=0, keepdims=True),
                           jnp.sum(a_t * wgt, axis=0, keepdims=True), jnp.sum(p_t, axis=0, keepdims=True))):
        out_ref[k:k + 1, :pos] = v


def exchange_kernel(n_dev, mine, out_ref, got, send_sem, recv_sem):
    me = lax.axis_index("tp")
    barrier = pltpu.get_barrier_semaphore()
    for d in range(1, n_dev):
        pl.semaphore_signal(barrier, inc=1, device_id={"tp": lax.rem(me + d, n_dev)}, device_id_type=MESH)
    got[me] = mine[...]
    pl.semaphore_wait(barrier, n_dev - 1)

    def send(d):
        return pltpu.make_async_remote_copy(
            src_ref=mine, dst_ref=got.at[me], send_sem=send_sem.at[d], recv_sem=recv_sem.at[me],
            device_id={"tp": lax.rem(me + d, n_dev)}, device_id_type=MESH)

    def arrive(d):
        peer = lax.rem(me + d, n_dev)
        return pltpu.make_async_remote_copy(
            src_ref=mine, dst_ref=got.at[peer], send_sem=send_sem.at[d], recv_sem=recv_sem.at[peer],
            device_id={"tp": peer}, device_id_type=MESH)

    sends = [send(d) for d in range(1, n_dev)]
    for c in sends:
        c.start()
    for d in range(1, n_dev):
        arrive(d).wait_recv()
    all_m = [got[d, 0:1, :] for d in range(n_dev)]
    top = functools.reduce(jnp.maximum, all_m)
    wgt = [jnp.exp(v - top) for v in all_m]
    out_ref[0:1, :] = top
    out_ref[1:2, :] = sum(got[d, 1:2, :] * wgt[d] for d in range(n_dev))
    out_ref[2:3, :] = sum(got[d, 2:3, :] * wgt[d] for d in range(n_dev))
    out_ref[3:4, :] = sum(got[d, 3:4, :] for d in range(n_dev))
    for c in sends:
        c.wait_send()


def solution(mesh):
    n_dev = mesh.shape["tp"]

    def local_part(hidden, norm_w, embedding, draft_ids):
        _, pos, width = hidden.shape
        hbm = pl.BlockSpec(memory_space=pltpu.HBM)
        vmem = pl.BlockSpec(memory_space=pltpu.VMEM)
        tile = pltpu.VMEM((8, LANES), jnp.float32)
        mine = pl.pallas_call(
            stream_kernel,
            out_shape=tile,
            in_specs=[hbm] * 4,
            out_specs=vmem,
            scratch_shapes=[
                pltpu.VMEM((1, pos, width), jnp.bfloat16),
                pltpu.VMEM((width // LANES, LANES), jnp.bfloat16),
                pltpu.VMEM((1, pos), jnp.int32),
                pltpu.VMEM((pos, width), jnp.bfloat16),
                pltpu.VMEM((DEPTH, BLOCK, width), jnp.bfloat16),
                pltpu.VMEM((pos, BLOCK), jnp.float32),
                pltpu.VMEM((4, pos, LANES), jnp.float32),
                pltpu.SemaphoreType.DMA((3,)),
                pltpu.SemaphoreType.DMA((DEPTH,)),
            ],
            compiler_params=pltpu.CompilerParams(vmem_limit_bytes=60 * 2**20),
            cost_estimate=pl.CostEstimate(flops=2 * pos * embedding.size, bytes_accessed=2 * embedding.size,
                                          transcendentals=pos * embedding.shape[0]),
            name="stream",
        )(hidden, norm_w.reshape(width // LANES, LANES), draft_ids, embedding)
        out = pl.pallas_call(
            functools.partial(exchange_kernel, n_dev),
            out_shape=tile,
            in_specs=[vmem],
            out_specs=vmem,
            scratch_shapes=[
                pltpu.VMEM((n_dev, 8, LANES), jnp.float32),
                pltpu.SemaphoreType.DMA((n_dev,)),
                pltpu.SemaphoreType.DMA((n_dev,)),
            ],
            compiler_params=pltpu.CompilerParams(collective_id=0, has_side_effects=True),
            name="exchange",
        )(mine)
        top, total, weighted, picked = (out[k:k + 1, :pos] for k in range(4))
        log_norm = top + jnp.log(total)
        return picked - log_norm, log_norm - weighted / total

    return jax.shard_map(local_part, mesh=mesh,
                         in_specs=(P("dp", None, None), P(None), P("tp", None), P("dp", None)),
                         out_specs=(P("dp", None), P("dp", None)), check_vma=False)
```

```python
import functools
import jax
import jax.numpy as jnp
from jax import lax
from jax.experimental import pallas as pl
from jax.experimental.pallas import tpu as pltpu
from jax.sharding import PartitionSpec as P

EPS = 1e-6
LANES = 128
BLOCK = 1280
DEPTH = 8
LOW = -3.0e38
MESH = pl.DeviceIdType.MESH


def stream_kernel(x_hbm, w_hbm, ids_hbm, e_hbm, out_ref,
                  x_ref, w_ref, ids_ref, h_ref, buf, z_ref, stat, small_sem, ring_sem):
    rows = e_hbm.shape[0]
    pos = x_ref.shape[1]
    steps = rows // BLOCK

    small = [pltpu.make_async_copy(s, d, small_sem.at[k])
             for k, (s, d) in enumerate(((x_hbm, x_ref), (w_hbm, w_ref), (ids_hbm, ids_ref)))]
    for c in small:
        c.start(priority=0)

    def fetch(i):
        slot = lax.rem(i, DEPTH)
        return pltpu.make_async_copy(e_hbm.at[pl.ds(i * BLOCK, BLOCK), :], buf.at[slot], ring_sem.at[slot])

    for i in range(DEPTH):
        fetch(i).start(priority=1)
    for c in small:
        c.wait()

    x = x_ref[0].astype(jnp.float32)
    r = lax.rsqrt(jnp.mean(x * x, axis=-1, keepdims=True) + EPS)
    gain = 1.0 + w_ref[...].astype(jnp.float32)
    for c in range(x.shape[1] // LANES):
        cols = slice(c * LANES, (c + 1) * LANES)
        h_ref[:, cols] = (x[:, cols] * r * gain[c:c + 1, :]).astype(jnp.bfloat16)

    sub = lax.broadcasted_iota(jnp.int32, (pos, pos), 0)
    lan = lax.broadcasted_iota(jnp.int32, (pos, pos), 1)
    ids_row = jnp.broadcast_to(ids_ref[...], (pos, pos)).astype(jnp.float32)
    ids_col = jnp.sum(jnp.where(sub == lan, ids_row, 0.0), axis=1, keepdims=True).astype(jnp.int32)
    ids_rel = ids_col - lax.axis_index("tp") * rows - lax.broadcasted_iota(jnp.int32, (pos, LANES), 1)

    stat[0] = jnp.full((pos, LANES), LOW, jnp.float32)
    for k in range(1, 4):
        stat[k] = jnp.zeros((pos, LANES), jnp.float32)

    def logits(i):
        return lax.dot_general(h_ref[...], buf[lax.rem(i, DEPTH)], (((1,), (1,)), ((), ())),
                               preferred_element_type=jnp.float32)

    def fold(i):
        tiles = [z_ref[:, j * LANES:(j + 1) * LANES] for j in range(BLOCK // LANES)]
        m_old = stat[0]
        m_new = functools.reduce(jnp.maximum, tiles, m_old)
        scale = jnp.exp(m_old - m_new)
        s, a, p = stat[1] * scale, stat[2] * scale, stat[3]
        for j, t in enumerate(tiles):
            e = jnp.exp(t - m_new)
            s += e
            a += e * t
            p += jnp.where(ids_rel == i * BLOCK + j * LANES, t, 0.0)
        stat[0], stat[1], stat[2], stat[3] = m_new, s, a, p

    fetch(0).wait()
    z_ref[...] = logits(0)

    def step(i, _):
        fetch(i).wait()
        nxt = i + DEPTH - 1

        @pl.when(nxt < steps)
        def _():
            fetch(nxt).start(priority=1)

        z = logits(i)
        fold(i - 1)
        z_ref[...] = z
        return 0

    lax.fori_loop(1, steps, step, 0)
    fold(steps - 1)

    m_t, s_t, a_t, p_t = stat[0].T, stat[1].T, stat[2].T, stat[3].T
    m = jnp.max(m_t, axis=0, keepdims=True)
    wgt = jnp.exp(m_t - m)
    for k, v in enumerate((m, jnp.sum(s_t * wgt, axis=0, keepdims=True),
                           jnp.sum(a_t * wgt, axis=0, keepdims=True), jnp.sum(p_t, axis=0, keepdims=True))):
        out_ref[k:k + 1, :pos] = v


def exchange_kernel(n_dev, mine, out_ref, got, send_sem, recv_sem):
    me = lax.axis_index("tp")
    barrier = pltpu.get_barrier_semaphore()
    for d in range(1, n_dev):
        pl.semaphore_signal(barrier, inc=1, device_id={"tp": lax.rem(me + d, n_dev)}, device_id_type=MESH)
    got[me] = mine[...]
    pl.semaphore_wait(barrier, n_dev - 1)

    def send(d):
        return pltpu.make_async_remote_copy(
            src_ref=mine, dst_ref=got.at[me], send_sem=send_sem.at[d], recv_sem=recv_sem.at[me],
            device_id={"tp": lax.rem(me + d, n_dev)}, device_id_type=MESH)

    def arrive(d):
        peer = lax.rem(me + d, n_dev)
        return pltpu.make_async_remote_copy(
            src_ref=mine, dst_ref=got.at[peer], send_sem=send_sem.at[d], recv_sem=recv_sem.at[peer],
            device_id={"tp": peer}, device_id_type=MESH)

    sends = [send(d) for d in range(1, n_dev)]
    for c in sends:
        c.start()
    for d in range(1, n_dev):
        arrive(d).wait_recv()
    all_m = [got[d, 0:1, :] for d in range(n_dev)]
    top = functools.reduce(jnp.maximum, all_m)
    wgt = [jnp.exp(v - top) for v in all_m]
    out_ref[0:1, :] = top
    out_ref[1:2, :] = sum(got[d, 1:2, :] * wgt[d] for d in range(n_dev))
    out_ref[2:3, :] = sum(got[d, 2:3, :] * wgt[d] for d in range(n_dev))
    out_ref[3:4, :] = sum(got[d, 3:4, :] for d in range(n_dev))
    for c in sends:
        c.wait_send()


def solution(mesh):
    n_dev = mesh.shape["tp"]

    def local_part(hidden, norm_w, embedding, draft_ids):
        _, pos, width = hidden.shape
        hbm = pl.BlockSpec(memory_space=pltpu.HBM)
        vmem = pl.BlockSpec(memory_space=pltpu.VMEM)
        tile = pltpu.VMEM((8, LANES), jnp.float32)
        mine = pl.pallas_call(
            stream_kernel,
            out_shape=tile,
            in_specs=[hbm] * 4,
            out_specs=vmem,
            scratch_shapes=[
                pltpu.VMEM((1, pos, width), jnp.bfloat16),
                pltpu.VMEM((width // LANES, LANES), jnp.bfloat16),
                pltpu.VMEM((1, pos), jnp.int32),
                pltpu.VMEM((pos, width), jnp.bfloat16),
                pltpu.VMEM((DEPTH, BLOCK, width), jnp.bfloat16),
                pltpu.VMEM((pos, BLOCK), jnp.float32),
                pltpu.VMEM((4, pos, LANES), jnp.float32),
                pltpu.SemaphoreType.DMA((3,)),
                pltpu.SemaphoreType.DMA((DEPTH,)),
            ],
            compiler_params=pltpu.CompilerParams(vmem_limit_bytes=60 * 2**20),
            cost_estimate=pl.CostEstimate(flops=2 * pos * embedding.size, bytes_accessed=2 * embedding.size,
                                          transcendentals=pos * embedding.shape[0]),
            name="stream",
        )(hidden, norm_w.reshape(width // LANES, LANES), draft_ids, embedding)
        out = pl.pallas_call(
            functools.partial(exchange_kernel, n_dev),
            out_shape=tile,
            in_specs=[vmem],
            out_specs=vmem,
            scratch_shapes=[
                pltpu.VMEM((n_dev, 8, LANES), jnp.float32),
                pltpu.SemaphoreType.DMA((n_dev,)),
                pltpu.SemaphoreType.DMA((n_dev,)),
            ],
            compiler_params=pltpu.CompilerParams(collective_id=0, has_side_effects=True),
            name="exchange",
        )(pltpu.with_memory_space_constraint(mine, pltpu.VMEM))
        top, total, weighted, picked = (out[k:k + 1, :pos] for k in range(4))
        log_norm = top + jnp.log(total)
        return picked - log_norm, log_norm - weighted / total

    return jax.shard_map(local_part, mesh=mesh,
                         in_specs=(P("dp", None, None), P(None), P("tp", None), P("dp", None)),
                         out_specs=(P("dp", None), P("dp", None)), check_vma=False)
```

```python
import functools
import jax
import jax.numpy as jnp
from jax import lax
from jax.experimental import pallas as pl
from jax.experimental.pallas import tpu as pltpu
from jax.sharding import PartitionSpec as P

EPS = 1e-6
LANES = 128
BLOCK = 512
TILE = 256
FLIP = 1024
DEPTH = 20
EARLY = 3
LOW = -3.0e38
MESH = pl.DeviceIdType.MESH


def head_kernel(n_dev, x_hbm, w_hbm, ids_hbm, e_hbm, out_ref,
                x_ref, w_ref, ids_ref, h_ref, odd, buf, flip, z_ref, stat, mine, got,
                small_sem, odd_sem, ring_sem, send_sem, recv_sem):
    rows, width = e_hbm.shape
    pos = x_ref.shape[1]
    lead = odd.shape[0]
    steps = (rows - lead) // BLOCK
    me = lax.axis_index("tp")
    barrier = pltpu.get_barrier_semaphore()

    small = [pltpu.make_async_copy(s, d, small_sem.at[k])
             for k, (s, d) in enumerate(((x_hbm, x_ref), (w_hbm, w_ref), (ids_hbm, ids_ref)))]
    first = pltpu.make_async_copy(e_hbm.at[pl.ds(0, lead), :], odd, odd_sem)

    def fetch(i):
        slot = lax.rem(i, DEPTH)
        return pltpu.make_async_copy(e_hbm.at[pl.ds(lead + i * BLOCK, BLOCK), :], buf.at[slot], ring_sem.at[slot])

    first.start()
    for i in range(EARLY):
        fetch(i).start()
    for c in small:
        c.start()
    for d in range(1, n_dev):
        pl.semaphore_signal(barrier, inc=1, device_id={"tp": lax.rem(me + d, n_dev)}, device_id_type=MESH)
    for c in small:
        c.wait()
    for i in range(EARLY, DEPTH):
        fetch(i).start()

    x = x_ref[0].astype(jnp.float32)
    r = lax.rsqrt(jnp.mean(x * x, axis=-1, keepdims=True) + EPS)
    gain = 1.0 + w_ref[...].astype(jnp.float32)
    for c in range(width // LANES):
        cols = slice(c * LANES, (c + 1) * LANES)
        h_ref[:, cols] = (x[:, cols] * r * gain[c:c + 1, :]).astype(jnp.bfloat16)

    sub = lax.broadcasted_iota(jnp.int32, (pos, pos), 0)
    lan = lax.broadcasted_iota(jnp.int32, (pos, pos), 1)
    ids_row = jnp.broadcast_to(ids_ref[...], (pos, pos)).astype(jnp.float32)
    ids_col = jnp.sum(jnp.where(sub == lan, ids_row, 0.0), axis=1, keepdims=True).astype(jnp.int32)
    ids_rel = ids_col - me * rows - lax.broadcasted_iota(jnp.int32, (pos, LANES), 1)

    stat[0] = jnp.full((pos, LANES), LOW, jnp.float32)
    for k in range(1, 4):
        stat[k] = jnp.zeros((pos, LANES), jnp.float32)

    def logits(src, count):
        out = []
        for j in range(count // TILE):
            part = pl.ds(j * TILE, TILE)
            turned = flip.at[j % 2]
            turned[...] = src[part, 0:FLIP].T
            z = jnp.dot(h_ref[:, 0:FLIP], turned[...], preferred_element_type=jnp.float32)
            z += lax.dot_general(h_ref[:, FLIP:], src[part, FLIP:], (((1,), (1,)), ((), ())),
                                 preferred_element_type=jnp.float32)
            out += [z[:, c * LANES:(c + 1) * LANES] for c in range(TILE // LANES)]
        return out

    def fold(tiles, start):
        m_old = stat[0]
        m_new = functools.reduce(jnp.maximum, tiles, m_old)
        scale = jnp.exp(m_old - m_new)
        s, a, p = stat[1] * scale, stat[2] * scale, stat[3]
        for j, t in enumerate(tiles):
            e = jnp.exp(t - m_new)
            s += e
            a += e * t
            p += jnp.where(ids_rel == start + j * LANES, t, 0.0)
        stat[0], stat[1], stat[2], stat[3] = m_new, s, a, p

    first.wait()
    fold(logits(odd, lead), 0)
    fetch(0).wait()
    for j, t in enumerate(logits(buf.at[0], BLOCK)):
        z_ref[j] = t

    def step(i, _):
        fetch(i).wait()
        nxt = i + DEPTH - 1

        @pl.when(nxt < steps)
        def _():
            fetch(nxt).start()

        tiles = logits(buf.at[lax.rem(i, DEPTH)], BLOCK)
        fold([z_ref[j] for j in range(BLOCK // LANES)], lead + (i - 1) * BLOCK)
        for j, t in enumerate(tiles):
            z_ref[j] = t
        return 0

    lax.fori_loop(1, steps, step, 0)
    fold([z_ref[j] for j in range(BLOCK // LANES)], lead + (steps - 1) * BLOCK)

    m_t, s_t, a_t, p_t = stat[0].T, stat[1].T, stat[2].T, stat[3].T
    m = jnp.max(m_t, axis=0, keepdims=True)
    wgt = jnp.exp(m_t - m)
    for k, v in enumerate((m, jnp.sum(s_t * wgt, axis=0, keepdims=True),
                           jnp.sum(a_t * wgt, axis=0, keepdims=True), jnp.sum(p_t, axis=0, keepdims=True))):
        mine[k:k + 1, :pos] = v
    got[me] = mine[...]
    pl.semaphore_wait(barrier, n_dev - 1)

    def send(d):
        return pltpu.make_async_remote_copy(
            src_ref=mine, dst_ref=got.at[me], send_sem=send_sem.at[d], recv_sem=recv_sem.at[me],
            device_id={"tp": lax.rem(me + d, n_dev)}, device_id_type=MESH)

    def arrive(d):
        peer = lax.rem(me + d, n_dev)
        return pltpu.make_async_remote_copy(
            src_ref=mine, dst_ref=got.at[peer], send_sem=send_sem.at[d], recv_sem=recv_sem.at[peer],
            device_id={"tp": peer}, device_id_type=MESH)

    sends = [send(d) for d in range(1, n_dev)]
    for c in sends:
        c.start()
    for d in range(1, n_dev):
        arrive(d).wait_recv()
    all_m = [got[d, 0:1, :pos] for d in range(n_dev)]
    top = functools.reduce(jnp.maximum, all_m)
    wgt = [jnp.exp(v - top) for v in all_m]
    out_ref[0:1, :pos] = top
    out_ref[1:2, :pos] = sum(got[d, 1:2, :pos] * wgt[d] for d in range(n_dev))
    out_ref[2:3, :pos] = sum(got[d, 2:3, :pos] * wgt[d] for d in range(n_dev))
    out_ref[3:4, :pos] = sum(got[d, 3:4, :pos] for d in range(n_dev))
    for c in sends:
        c.wait_send()


def solution(mesh):
    n_dev = mesh.shape["tp"]

    def local_part(hidden, norm_w, embedding, draft_ids):
        _, pos, width = hidden.shape
        hbm = pl.BlockSpec(memory_space=pltpu.HBM)
        vmem = pl.BlockSpec(memory_space=pltpu.VMEM)
        out = pl.pallas_call(
            functools.partial(head_kernel, n_dev),
            out_shape=pltpu.VMEM((8, LANES), jnp.float32),
            in_specs=[hbm] * 4,
            out_specs=vmem,
            scratch_shapes=[
                pltpu.VMEM((1, pos, width), jnp.bfloat16),
                pltpu.VMEM((width // LANES, LANES), jnp.bfloat16),
                pltpu.VMEM((1, pos), jnp.int32),
                pltpu.VMEM((pos, width), jnp.bfloat16),
                pltpu.VMEM((embedding.shape[0] % BLOCK, width), jnp.bfloat16),
                pltpu.VMEM((DEPTH, BLOCK, width), jnp.bfloat16),
                pltpu.VMEM((2, FLIP, TILE), jnp.bfloat16),
                pltpu.VMEM((BLOCK // LANES, pos, LANES), jnp.float32),
                pltpu.VMEM((4, pos, LANES), jnp.float32),
                pltpu.VMEM((8, LANES), jnp.float32),
                pltpu.VMEM((n_dev, 8, LANES), jnp.float32),
                pltpu.SemaphoreType.DMA((3,)),
                pltpu.SemaphoreType.DMA,
                pltpu.SemaphoreType.DMA((DEPTH,)),
                pltpu.SemaphoreType.DMA((n_dev,)),
                pltpu.SemaphoreType.DMA((n_dev,)),
            ],
            compiler_params=pltpu.CompilerParams(
                collective_id=0, has_side_effects=True, vmem_limit_bytes=60 * 2**20),
            cost_estimate=pl.CostEstimate(flops=2 * pos * embedding.size, bytes_accessed=2 * embedding.size,
                                          transcendentals=pos * embedding.shape[0]),
            name="head",
        )(hidden, norm_w.reshape(width // LANES, LANES), draft_ids, embedding)
        top, total, weighted, picked = (out[k:k + 1, :pos] for k in range(4))
        log_norm = top + jnp.log(total)
        return picked - log_norm, log_norm - weighted / total

    return jax.shard_map(local_part, mesh=mesh,
                         in_specs=(P("dp", None, None), P(None), P("tp", None), P("dp", None)),
                         out_specs=(P("dp", None), P("dp", None)), check_vma=False)
```

```python
import functools
import jax
import jax.numpy as jnp
from jax import lax
from jax.experimental import pallas as pl
from jax.experimental.pallas import tpu as pltpu
from jax.sharding import PartitionSpec as P

EPS = 1e-6
LANES = 128
BLOCK = 512
TILE = 256
FLIP = 1024
DEPTH = 20
LOW = -3.0e38
MESH = pl.DeviceIdType.MESH


def head_kernel(n_dev, x_hbm, w_hbm, ids_hbm, e_hbm, out_ref,
                x_ref, w_ref, ids_ref, h_ref, odd, buf, flip, z_ref, stat, mine, got,
                small_sem, odd_sem, ring_sem, send_sem, recv_sem):
    rows, width = e_hbm.shape
    pos = x_ref.shape[1]
    lead = odd.shape[0]
    steps = (rows - lead) // BLOCK
    me = lax.axis_index("tp")
    barrier = pltpu.get_barrier_semaphore()

    small = [pltpu.make_async_copy(s, d, small_sem.at[k])
             for k, (s, d) in enumerate(((x_hbm, x_ref), (w_hbm, w_ref), (ids_hbm, ids_ref)))]
    first = pltpu.make_async_copy(e_hbm.at[pl.ds(0, lead), :], odd, odd_sem)

    def fetch(i):
        slot = lax.rem(i, DEPTH)
        return pltpu.make_async_copy(e_hbm.at[pl.ds(lead + i * BLOCK, BLOCK), :], buf.at[slot], ring_sem.at[slot])

    for c in small:
        c.start()

    def prime(i, _):
        @pl.when(i == 0)
        def _():
            first.start()

        fetch(i).start()
        return 0

    lax.fori_loop(0, DEPTH, prime, 0)
    for d in range(1, n_dev):
        pl.semaphore_signal(barrier, inc=1, device_id={"tp": lax.rem(me + d, n_dev)}, device_id_type=MESH)
    for c in small:
        c.wait()

    x = x_ref[0].astype(jnp.float32)
    r = lax.rsqrt(jnp.mean(x * x, axis=-1, keepdims=True) + EPS)
    gain = 1.0 + w_ref[...].astype(jnp.float32)
    for c in range(width // LANES):
        cols = slice(c * LANES, (c + 1) * LANES)
        h_ref[:, cols] = (x[:, cols] * r * gain[c:c + 1, :]).astype(jnp.bfloat16)

    sub = lax.broadcasted_iota(jnp.int32, (pos, pos), 0)
    lan = lax.broadcasted_iota(jnp.int32, (pos, pos), 1)
    ids_row = jnp.broadcast_to(ids_ref[...], (pos, pos)).astype(jnp.float32)
    ids_col = jnp.sum(jnp.where(sub == lan, ids_row, 0.0), axis=1, keepdims=True).astype(jnp.int32)
    ids_rel = ids_col - me * rows - lax.broadcasted_iota(jnp.int32, (pos, LANES), 1)

    stat[0] = jnp.full((pos, LANES), LOW, jnp.float32)
    for k in range(1, 4):
        stat[k] = jnp.zeros((pos, LANES), jnp.float32)

    def logits(src, count):
        out = []
        for j in range(count // TILE):
            part = pl.ds(j * TILE, TILE)
            turned = flip.at[j % 2]
            turned[...] = src[part, 0:FLIP].T
            z = jnp.dot(h_ref[:, 0:FLIP], turned[...], preferred_element_type=jnp.float32)
            z += lax.dot_general(h_ref[:, FLIP:], src[part, FLIP:], (((1,), (1,)), ((), ())),
                                 preferred_element_type=jnp.float32)
            out += [z[:, c * LANES:(c + 1) * LANES] for c in range(TILE // LANES)]
        return out

    def fold(tiles, start):
        m_old = stat[0]
        m_new = functools.reduce(jnp.maximum, tiles, m_old)
        scale = jnp.exp(m_old - m_new)
        s, a, p = stat[1] * scale, stat[2] * scale, stat[3]
        for j, t in enumerate(tiles):
            e = jnp.exp(t - m_new)
            s += e
            a += e * t
            p += jnp.where(ids_rel == start + j * LANES, t, 0.0)
        stat[0], stat[1], stat[2], stat[3] = m_new, s, a, p

    first.wait()
    fold(logits(odd, lead), 0)
    fetch(0).wait()
    for j, t in enumerate(logits(buf.at[0], BLOCK)):
        z_ref[j] = t

    def step(i, _):
        fetch(i).wait()
        nxt = i + DEPTH - 1

        @pl.when(nxt < steps)
        def _():
            fetch(nxt).start()

        tiles = logits(buf.at[lax.rem(i, DEPTH)], BLOCK)
        fold([z_ref[j] for j in range(BLOCK // LANES)], lead + (i - 1) * BLOCK)
        for j, t in enumerate(tiles):
            z_ref[j] = t
        return 0

    lax.fori_loop(1, steps, step, 0)
    fold([z_ref[j] for j in range(BLOCK // LANES)], lead + (steps - 1) * BLOCK)

    m_t, s_t, a_t, p_t = stat[0].T, stat[1].T, stat[2].T, stat[3].T
    m = jnp.max(m_t, axis=0, keepdims=True)
    wgt = jnp.exp(m_t - m)
    for k, v in enumerate((m, jnp.sum(s_t * wgt, axis=0, keepdims=True),
                           jnp.sum(a_t * wgt, axis=0, keepdims=True), jnp.sum(p_t, axis=0, keepdims=True))):
        mine[k:k + 1, :pos] = v
    got[me] = mine[...]
    pl.semaphore_wait(barrier, n_dev - 1)

    def send(d):
        return pltpu.make_async_remote_copy(
            src_ref=mine, dst_ref=got.at[me], send_sem=send_sem.at[d], recv_sem=recv_sem.at[me],
            device_id={"tp": lax.rem(me + d, n_dev)}, device_id_type=MESH)

    def arrive(d):
        peer = lax.rem(me + d, n_dev)
        return pltpu.make_async_remote_copy(
            src_ref=mine, dst_ref=got.at[peer], send_sem=send_sem.at[d], recv_sem=recv_sem.at[peer],
            device_id={"tp": peer}, device_id_type=MESH)

    sends = [send(d) for d in range(1, n_dev)]
    for c in sends:
        c.start()
    for d in range(1, n_dev):
        arrive(d).wait_recv()
    all_m = [got[d, 0:1, :pos] for d in range(n_dev)]
    top = functools.reduce(jnp.maximum, all_m)
    wgt = [jnp.exp(v - top) for v in all_m]
    out_ref[0:1, :pos] = top
    out_ref[1:2, :pos] = sum(got[d, 1:2, :pos] * wgt[d] for d in range(n_dev))
    out_ref[2:3, :pos] = sum(got[d, 2:3, :pos] * wgt[d] for d in range(n_dev))
    out_ref[3:4, :pos] = sum(got[d, 3:4, :pos] for d in range(n_dev))
    for c in sends:
        c.wait_send()


def solution(mesh):
    n_dev = mesh.shape["tp"]

    def local_part(hidden, norm_w, embedding, draft_ids):
        _, pos, width = hidden.shape
        hbm = pl.BlockSpec(memory_space=pltpu.HBM)
        vmem = pl.BlockSpec(memory_space=pltpu.VMEM)
        out = pl.pallas_call(
            functools.partial(head_kernel, n_dev),
            out_shape=pltpu.VMEM((8, LANES), jnp.float32),
            in_specs=[hbm] * 4,
            out_specs=vmem,
            scratch_shapes=[
                pltpu.VMEM((1, pos, width), jnp.bfloat16),
                pltpu.VMEM((width // LANES, LANES), jnp.bfloat16),
                pltpu.VMEM((1, pos), jnp.int32),
                pltpu.VMEM((pos, width), jnp.bfloat16),
                pltpu.VMEM((embedding.shape[0] % BLOCK, width), jnp.bfloat16),
                pltpu.VMEM((DEPTH, BLOCK, width), jnp.bfloat16),
                pltpu.VMEM((2, FLIP, TILE), jnp.bfloat16),
                pltpu.VMEM((BLOCK // LANES, pos, LANES), jnp.float32),
                pltpu.VMEM((4, pos, LANES), jnp.float32),
                pltpu.VMEM((8, LANES), jnp.float32),
                pltpu.VMEM((n_dev, 8, LANES), jnp.float32),
                pltpu.SemaphoreType.DMA((3,)),
                pltpu.SemaphoreType.DMA,
                pltpu.SemaphoreType.DMA((DEPTH,)),
                pltpu.SemaphoreType.DMA((n_dev,)),
                pltpu.SemaphoreType.DMA((n_dev,)),
            ],
            compiler_params=pltpu.CompilerParams(
                collective_id=0, has_side_effects=True, vmem_limit_bytes=60 * 2**20),
            cost_estimate=pl.CostEstimate(flops=2 * pos * embedding.size, bytes_accessed=2 * embedding.size,
                                          transcendentals=pos * embedding.shape[0]),
            name="head",
        )(hidden, norm_w.reshape(width // LANES, LANES), draft_ids, embedding)
        top, total, weighted, picked = (out[k:k + 1, :pos] for k in range(4))
        log_norm = top + jnp.log(total)
        return picked - log_norm, log_norm - weighted / total

    return jax.shard_map(local_part, mesh=mesh,
                         in_specs=(P("dp", None, None), P(None), P("tp", None), P("dp", None)),
                         out_specs=(P("dp", None), P("dp", None)), check_vma=False)
```

```python
import functools
import jax
import jax.numpy as jnp
from jax import lax
from jax.experimental import pallas as pl
from jax.experimental.pallas import tpu as pltpu
from jax.sharding import PartitionSpec as P

EPS = 1e-6
LANES = 128
BLOCK = 384
FLIP = 1024
DEPTH = 10
LOW = -3.0e38
MESH = pl.DeviceIdType.MESH


def farthest_first(me, n_dev):
    if n_dev != 8:
        return [lax.rem(me + d, n_dev) for d in range(1, n_dev)]
    y, x, core = me // 4, (me // 2) % 2, me % 2
    flipped = [(1, 1, 0), (1, 1, 1), (1, 0, 0), (0, 1, 0), (1, 0, 1), (0, 1, 1), (0, 0, 1)]
    return [(1 - y if a else y) * 4 + (1 - x if b else x) * 2 + (1 - core if c else core) for a, b, c in flipped]


def head_kernel(n_dev, x_hbm, w_hbm, ids_hbm, e_hbm, out_ref,
                x_ref, w_ref, ids_ref, h_ref, odd, buf, flip, z_ref, stat, mine, got,
                ring_sem, side_sem, recv_sem):
    rows, width = e_hbm.shape
    pos = x_ref.shape[1]
    lead = odd.shape[0]
    steps = (rows - lead) // BLOCK
    me = lax.axis_index("tp")
    barrier = pltpu.get_barrier_semaphore()

    small = [pltpu.make_async_copy(s, d, side_sem.at[k])
             for k, (s, d) in enumerate(((x_hbm, x_ref), (w_hbm, w_ref), (ids_hbm, ids_ref)))]
    first = pltpu.make_async_copy(e_hbm.at[pl.ds(0, lead), :], odd, side_sem.at[3])

    def fetch(i):
        slot = lax.rem(i, DEPTH)
        return pltpu.make_async_copy(e_hbm.at[pl.ds(lead + i * BLOCK, BLOCK), :], buf.at[slot], ring_sem.at[slot])

    for c in small:
        c.start()

    def prime(i, _):
        @pl.when(i == 0)
        def _():
            first.start()

        fetch(i).start()
        return 0

    lax.fori_loop(0, DEPTH, prime, 0)
    for d in range(1, n_dev):
        pl.semaphore_signal(barrier, inc=1, device_id={"tp": lax.rem(me + d, n_dev)}, device_id_type=MESH)
    for c in small:
        c.wait()

    x = x_ref[0].astype(jnp.float32)
    r = lax.rsqrt(jnp.mean(x * x, axis=-1, keepdims=True) + EPS)
    gain = 1.0 + w_ref[...].astype(jnp.float32)
    for c in range(width // LANES):
        cols = slice(c * LANES, (c + 1) * LANES)
        h_ref[:, cols] = (x[:, cols] * r * gain[c:c + 1, :]).astype(jnp.bfloat16)

    sub = lax.broadcasted_iota(jnp.int32, (pos, pos), 0)
    lan = lax.broadcasted_iota(jnp.int32, (pos, pos), 1)
    ids_row = jnp.broadcast_to(ids_ref[...], (pos, pos)).astype(jnp.float32)
    ids_col = jnp.sum(jnp.where(sub == lan, ids_row, 0.0), axis=1, keepdims=True).astype(jnp.int32)
    ids_rel = ids_col - me * rows - lax.broadcasted_iota(jnp.int32, (pos, LANES), 1)

    stat[0] = jnp.full((pos, LANES), LOW, jnp.float32)
    for k in range(1, 4):
        stat[k] = jnp.zeros((pos, LANES), jnp.float32)

    def logits(src, count):
        turned = flip.at[:, 0:count]
        turned[...] = src[:, 0:FLIP].T
        z = jnp.dot(h_ref[:, 0:FLIP], turned[...], preferred_element_type=jnp.float32)
        z += lax.dot_general(h_ref[:, FLIP:], src[:, FLIP:], (((1,), (1,)), ((), ())),
                             preferred_element_type=jnp.float32)
        return [z[:, c:c + LANES] for c in range(0, count, LANES)]

    def fold(tiles, start):
        m_old = stat[0]
        m_new = functools.reduce(jnp.maximum, tiles, m_old)
        scale = jnp.exp(m_old - m_new)
        s, a, p = stat[1] * scale, stat[2] * scale, stat[3]
        for j, t in enumerate(tiles):
            e = jnp.exp(t - m_new)
            s += e
            a += e * t
            p += jnp.where(ids_rel == start + j * LANES, t, 0.0)
        stat[0], stat[1], stat[2], stat[3] = m_new, s, a, p

    first.wait()
    fold(logits(odd, lead), 0)
    fetch(0).wait()
    for j, t in enumerate(logits(buf.at[0], BLOCK)):
        z_ref[j] = t

    def step(i, _):
        fetch(i).wait()
        nxt = i + DEPTH - 1

        @pl.when(nxt < steps)
        def _():
            fetch(nxt).start()

        tiles = logits(buf.at[lax.rem(i, DEPTH)], BLOCK)
        fold([z_ref[j] for j in range(BLOCK // LANES)], lead + (i - 1) * BLOCK)
        for j, t in enumerate(tiles):
            z_ref[j] = t
        return 0

    lax.fori_loop(1, steps, step, 0)
    fold([z_ref[j] for j in range(BLOCK // LANES)], lead + (steps - 1) * BLOCK)

    m_t, s_t, a_t, p_t = stat[0].T, stat[1].T, stat[2].T, stat[3].T
    m = jnp.max(m_t, axis=0, keepdims=True)
    wgt = jnp.exp(m_t - m)
    for k, v in enumerate((m, jnp.sum(s_t * wgt, axis=0, keepdims=True),
                           jnp.sum(a_t * wgt, axis=0, keepdims=True), jnp.sum(p_t, axis=0, keepdims=True))):
        mine[k:k + 1, :pos] = v
    got[me] = mine[...]
    pl.semaphore_wait(barrier, n_dev - 1)

    def send(peer):
        return pltpu.make_async_remote_copy(
            src_ref=mine, dst_ref=got.at[me], send_sem=side_sem.at[0], recv_sem=recv_sem,
            device_id={"tp": peer}, device_id_type=MESH)

    for peer in farthest_first(me, n_dev):
        send(peer).start()
    others = got.at[pl.ds(0, n_dev - 1)]
    exchange = pltpu.make_async_remote_copy(
        src_ref=others, dst_ref=others, send_sem=side_sem.at[0], recv_sem=recv_sem,
        device_id={"tp": me}, device_id_type=MESH)
    exchange.wait_recv()
    all_m = [got[d, 0:1, :pos] for d in range(n_dev)]
    top = functools.reduce(jnp.maximum, all_m)
    wgt = [jnp.exp(v - top) for v in all_m]
    out_ref[0:1, :pos] = top
    out_ref[1:2, :pos] = sum(got[d, 1:2, :pos] * wgt[d] for d in range(n_dev))
    out_ref[2:3, :pos] = sum(got[d, 2:3, :pos] * wgt[d] for d in range(n_dev))
    out_ref[3:4, :pos] = sum(got[d, 3:4, :pos] for d in range(n_dev))
    exchange.wait_send()


def solution(mesh):
    n_dev = mesh.shape["tp"]

    def local_part(hidden, norm_w, embedding, draft_ids):
        _, pos, width = hidden.shape
        hbm = pl.BlockSpec(memory_space=pltpu.HBM)
        vmem = pl.BlockSpec(memory_space=pltpu.VMEM)
        out = pl.pallas_call(
            functools.partial(head_kernel, n_dev),
            out_shape=pltpu.VMEM((4, LANES), jnp.float32),
            in_specs=[hbm] * 4,
            out_specs=vmem,
            scratch_shapes=[
                pltpu.VMEM((1, pos, width), jnp.bfloat16),
                pltpu.VMEM((width // LANES, LANES), jnp.bfloat16),
                pltpu.VMEM((1, pos), jnp.int32),
                pltpu.VMEM((pos, width), jnp.bfloat16),
                pltpu.VMEM((embedding.shape[0] % BLOCK, width), jnp.bfloat16),
                pltpu.VMEM((DEPTH, BLOCK, width), jnp.bfloat16),
                pltpu.VMEM((FLIP, BLOCK), jnp.bfloat16),
                pltpu.VMEM((BLOCK // LANES, pos, LANES), jnp.float32),
                pltpu.VMEM((4, pos, LANES), jnp.float32),
                pltpu.VMEM((4, LANES), jnp.float32),
                pltpu.VMEM((n_dev, 4, LANES), jnp.float32),
                pltpu.SemaphoreType.DMA((DEPTH,)),
                pltpu.SemaphoreType.DMA((4,)),
                pltpu.SemaphoreType.DMA,
            ],
            compiler_params=pltpu.CompilerParams(
                collective_id=0, has_side_effects=True, vmem_limit_bytes=60 * 2**20),
            cost_estimate=pl.CostEstimate(flops=2 * pos * embedding.size, bytes_accessed=2 * embedding.size,
                                          transcendentals=pos * embedding.shape[0]),
            name="head",
        )(hidden, norm_w.reshape(width // LANES, LANES), draft_ids, embedding)
        top, total, weighted, picked = (out[k:k + 1, :pos] for k in range(4))
        log_norm = top + jnp.log(total)
        return picked - log_norm, log_norm - weighted / total

    return jax.shard_map(local_part, mesh=mesh,
                         in_specs=(P("dp", None, None), P(None), P("tp", None), P("dp", None)),
                         out_specs=(P("dp", None), P("dp", None)), check_vma=False)
```

```python
import functools
import jax
import jax.numpy as jnp
from jax import lax
from jax.experimental import pallas as pl
from jax.experimental.pallas import tpu as pltpu
from jax.sharding import PartitionSpec as P

EPS = 1e-6
LANES = 128
BLOCK = 384
FLIP = 1024
DEPTH = 8
LOW = -3.0e38
MESH = pl.DeviceIdType.MESH


def tree(op, values):
    while len(values) > 1:
        values = [op(*values[k:k + 2]) if k + 1 < len(values) else values[k] for k in range(0, len(values), 2)]
    return values[0]


def farthest_first(me, n_dev):
    if n_dev != 8:
        return [lax.rem(me + d, n_dev) for d in range(1, n_dev)]
    y, x, core = me // 4, (me // 2) % 2, me % 2
    flipped = [(1, 1, 0), (1, 1, 1), (1, 0, 0), (0, 1, 0), (1, 0, 1), (0, 1, 1), (0, 0, 1)]
    return [(1 - y if a else y) * 4 + (1 - x if b else x) * 2 + (1 - core if c else core) for a, b, c in flipped]


def head_kernel(n_dev, x_hbm, w_hbm, ids_hbm, e_hbm, out_ref,
                x_ref, w_ref, ids_ref, h_ref, odd, buf, flip, z_ref, stat, mine, got,
                ring_sem, side_sem, recv_sem):
    rows, width = e_hbm.shape
    pos = x_ref.shape[1]
    lead = odd.shape[0]
    steps = (rows - lead) // BLOCK
    me = lax.axis_index("tp")
    barrier = pltpu.get_barrier_semaphore()

    small = [pltpu.make_async_copy(s, d, side_sem.at[k])
             for k, (s, d) in enumerate(((x_hbm, x_ref), (w_hbm, w_ref), (ids_hbm, ids_ref)))]
    first = pltpu.make_async_copy(e_hbm.at[pl.ds(0, lead), :], odd, side_sem.at[3])

    def fetch(i):
        slot = lax.rem(i, DEPTH)
        return pltpu.make_async_copy(e_hbm.at[pl.ds(lead + i * BLOCK, BLOCK), :], buf.at[slot], ring_sem.at[slot])

    first.start()
    fetch(0).start()
    for c in small:
        c.start()

    def prime(i, _):
        fetch(i).start()
        return 0

    lax.fori_loop(1, DEPTH, prime, 0)
    for d in range(1, n_dev):
        pl.semaphore_signal(barrier, inc=1, device_id={"tp": lax.rem(me + d, n_dev)}, device_id_type=MESH)
    for c in small:
        c.wait()

    x = x_ref[0].astype(jnp.float32)
    r = lax.rsqrt(jnp.mean(x * x, axis=-1, keepdims=True) + EPS)
    gain = 1.0 + w_ref[...].astype(jnp.float32)
    for c in range(width // LANES):
        cols = slice(c * LANES, (c + 1) * LANES)
        h_ref[:, cols] = (x[:, cols] * r * gain[c:c + 1, :]).astype(jnp.bfloat16)

    sub = lax.broadcasted_iota(jnp.int32, (pos, pos), 0)
    lan = lax.broadcasted_iota(jnp.int32, (pos, pos), 1)
    ids_row = jnp.broadcast_to(ids_ref[...], (pos, pos)).astype(jnp.float32)
    ids_col = jnp.sum(jnp.where(sub == lan, ids_row, 0.0), axis=1, keepdims=True).astype(jnp.int32)
    ids_rel = ids_col - me * rows - lax.broadcasted_iota(jnp.int32, (pos, LANES), 1)

    stat[0] = jnp.full((pos, LANES), LOW, jnp.float32)
    for k in range(1, 4):
        stat[k] = jnp.zeros((pos, LANES), jnp.float32)

    def logits(src, count):
        turned = flip.at[:, 0:count]
        turned[...] = src[:, 0:FLIP].T
        z = jnp.dot(h_ref[:, 0:FLIP], turned[...], preferred_element_type=jnp.float32)
        z += lax.dot_general(h_ref[:, FLIP:], src[:, FLIP:], (((1,), (1,)), ((), ())),
                             preferred_element_type=jnp.float32)
        return [z[:, c:c + LANES] for c in range(0, count, LANES)]

    def fold(tiles, start):
        m_old = stat[0]
        m_new = tree(jnp.maximum, [m_old] + tiles)
        scale = jnp.exp(m_old - m_new)
        parts = [jnp.exp(t - m_new) for t in tiles]
        stat[0] = m_new
        stat[1] = tree(jnp.add, [stat[1] * scale] + parts)
        stat[2] = tree(jnp.add, [stat[2] * scale] + [e * t for e, t in zip(parts, tiles)])
        stat[3] = tree(jnp.add, [stat[3]] + [jnp.where(ids_rel == start + j * LANES, t, 0.0)
                                             for j, t in enumerate(tiles)])

    first.wait()
    fold(logits(odd, lead), 0)
    fetch(0).wait()
    for j, t in enumerate(logits(buf.at[0], BLOCK)):
        z_ref[j] = t

    def step(i, _):
        fetch(i).wait()
        nxt = i + DEPTH - 1

        @pl.when(nxt < steps)
        def _():
            fetch(nxt).start()

        tiles = logits(buf.at[lax.rem(i, DEPTH)], BLOCK)
        fold([z_ref[j] for j in range(BLOCK // LANES)], lead + (i - 1) * BLOCK)
        for j, t in enumerate(tiles):
            z_ref[j] = t
        return 0

    lax.fori_loop(1, steps, step, 0)
    fold([z_ref[j] for j in range(BLOCK // LANES)], lead + (steps - 1) * BLOCK)

    m_t, s_t, a_t, p_t = stat[0].T, stat[1].T, stat[2].T, stat[3].T
    m = jnp.max(m_t, axis=0, keepdims=True)
    wgt = jnp.exp(m_t - m)
    for k, v in enumerate((m, jnp.sum(s_t * wgt, axis=0, keepdims=True),
                           jnp.sum(a_t * wgt, axis=0, keepdims=True), jnp.sum(p_t, axis=0, keepdims=True))):
        mine[k:k + 1, :pos] = v
    got[me] = mine[...]
    pl.semaphore_wait(barrier, n_dev - 1)

    def send(peer):
        return pltpu.make_async_remote_copy(
            src_ref=mine, dst_ref=got.at[me], send_sem=side_sem.at[0], recv_sem=recv_sem,
            device_id={"tp": peer}, device_id_type=MESH)

    for peer in farthest_first(me, n_dev):
        send(peer).start()
    others = got.at[pl.ds(0, n_dev - 1)]
    exchange = pltpu.make_async_remote_copy(
        src_ref=others, dst_ref=others, send_sem=side_sem.at[0], recv_sem=recv_sem,
        device_id={"tp": me}, device_id_type=MESH)
    exchange.wait_recv()
    all_m = [got[d, 0:1, :pos] for d in range(n_dev)]
    top = tree(jnp.maximum, all_m)
    wgt = [jnp.exp(v - top) for v in all_m]
    out_ref[0:1, :pos] = top
    out_ref[1:2, :pos] = tree(jnp.add, [got[d, 1:2, :pos] * wgt[d] for d in range(n_dev)])
    out_ref[2:3, :pos] = tree(jnp.add, [got[d, 2:3, :pos] * wgt[d] for d in range(n_dev)])
    out_ref[3:4, :pos] = tree(jnp.add, [got[d, 3:4, :pos] for d in range(n_dev)])
    exchange.wait_send()


def solution(mesh):
    n_dev = mesh.shape["tp"]

    def local_part(hidden, norm_w, embedding, draft_ids):
        _, pos, width = hidden.shape
        hbm = pl.BlockSpec(memory_space=pltpu.HBM)
        vmem = pl.BlockSpec(memory_space=pltpu.VMEM)
        out = pl.pallas_call(
            functools.partial(head_kernel, n_dev),
            out_shape=pltpu.VMEM((4, LANES), jnp.float32),
            in_specs=[hbm] * 4,
            out_specs=vmem,
            scratch_shapes=[
                pltpu.VMEM((1, pos, width), jnp.bfloat16),
                pltpu.VMEM((width // LANES, LANES), jnp.bfloat16),
                pltpu.VMEM((1, pos), jnp.int32),
                pltpu.VMEM((pos, width), jnp.bfloat16),
                pltpu.VMEM((embedding.shape[0] % BLOCK, width), jnp.bfloat16),
                pltpu.VMEM((DEPTH, BLOCK, width), jnp.bfloat16),
                pltpu.VMEM((FLIP, BLOCK), jnp.bfloat16),
                pltpu.VMEM((BLOCK // LANES, pos, LANES), jnp.float32),
                pltpu.VMEM((4, pos, LANES), jnp.float32),
                pltpu.VMEM((4, LANES), jnp.float32),
                pltpu.VMEM((n_dev, 4, LANES), jnp.float32),
                pltpu.SemaphoreType.DMA((DEPTH,)),
                pltpu.SemaphoreType.DMA((4,)),
                pltpu.SemaphoreType.DMA,
            ],
            compiler_params=pltpu.CompilerParams(
                collective_id=0, has_side_effects=True, vmem_limit_bytes=60 * 2**20),
            cost_estimate=pl.CostEstimate(flops=2 * pos * embedding.size, bytes_accessed=2 * embedding.size,
                                          transcendentals=pos * embedding.shape[0]),
            name="head",
        )(hidden, norm_w.reshape(width // LANES, LANES), draft_ids, embedding)
        top, total, weighted, picked = (out[k:k + 1, :pos] for k in range(4))
        log_norm = top + jnp.log(total)
        return picked - log_norm, log_norm - weighted / total

    return jax.shard_map(local_part, mesh=mesh,
                         in_specs=(P("dp", None, None), P(None), P("tp", None), P("dp", None)),
                         out_specs=(P("dp", None), P("dp", None)), check_vma=False)
```

```python
import functools
import jax
import jax.numpy as jnp
from jax import lax
from jax.experimental import pallas as pl
from jax.experimental.pallas import tpu as pltpu
from jax.sharding import PartitionSpec as P

EPS = 1e-6
LANES = 128
BLOCK = 384
FLIP = 1024
DEPTH = 8
LOW = -3.0e38
MESH = pl.DeviceIdType.MESH


def tree(op, values):
    while len(values) > 1:
        values = [op(*values[k:k + 2]) if k + 1 < len(values) else values[k] for k in range(0, len(values), 2)]
    return values[0]


def farthest_first(me, n_dev):
    if n_dev != 8:
        return [lax.rem(me + d, n_dev) for d in range(1, n_dev)]
    y, x, core = me // 4, (me // 2) % 2, me % 2
    flipped = [(1, 1, 0), (1, 1, 1), (1, 0, 0), (0, 1, 0), (1, 0, 1), (0, 1, 1), (0, 0, 1)]
    return [(1 - y if a else y) * 4 + (1 - x if b else x) * 2 + (1 - core if c else core) for a, b, c in flipped]


def head_kernel(n_dev, *refs):
    pl.run_scoped(functools.partial(head_body, n_dev, *refs),
                  pltpu.SemaphoreType.DMA((DEPTH,)), pltpu.SemaphoreType.DMA((4,)))


def head_body(n_dev, x_hbm, w_hbm, ids_hbm, e_hbm, out_ref,
              x_ref, w_ref, ids_ref, h_ref, odd, buf, flip, z_ref, stat, mine, got, recv_sem,
              ring_sem, side_sem):
    rows, width = e_hbm.shape
    pos = x_ref.shape[1]
    lead = odd.shape[0]
    steps = (rows - lead) // BLOCK
    me = lax.axis_index("tp")
    barrier = pltpu.get_barrier_semaphore()

    small = [pltpu.make_async_copy(s, d, side_sem.at[k])
             for k, (s, d) in enumerate(((x_hbm, x_ref), (w_hbm, w_ref), (ids_hbm, ids_ref)))]
    first = pltpu.make_async_copy(e_hbm.at[pl.ds(0, lead), :], odd, side_sem.at[3])

    def fetch(i):
        slot = lax.rem(i, DEPTH)
        return pltpu.make_async_copy(e_hbm.at[pl.ds(lead + i * BLOCK, BLOCK), :], buf.at[slot], ring_sem.at[slot])

    first.start()
    fetch(0).start()
    for c in small:
        c.start()

    def prime(i, _):
        fetch(i).start()
        return 0

    lax.fori_loop(1, DEPTH, prime, 0)
    for d in range(1, n_dev):
        pl.semaphore_signal(barrier, inc=1, device_id={"tp": lax.rem(me + d, n_dev)}, device_id_type=MESH)
    for c in small:
        c.wait()

    x = x_ref[0].astype(jnp.float32)
    r = lax.rsqrt(jnp.mean(x * x, axis=-1, keepdims=True) + EPS)
    gain = 1.0 + w_ref[...].astype(jnp.float32)
    for c in range(width // LANES):
        cols = slice(c * LANES, (c + 1) * LANES)
        h_ref[:, cols] = (x[:, cols] * r * gain[c:c + 1, :]).astype(jnp.bfloat16)

    sub = lax.broadcasted_iota(jnp.int32, (pos, pos), 0)
    lan = lax.broadcasted_iota(jnp.int32, (pos, pos), 1)
    ids_row = jnp.broadcast_to(ids_ref[...], (pos, pos)).astype(jnp.float32)
    ids_col = jnp.sum(jnp.where(sub == lan, ids_row, 0.0), axis=1, keepdims=True).astype(jnp.int32)
    ids_rel = ids_col - me * rows - lax.broadcasted_iota(jnp.int32, (pos, LANES), 1)

    stat[0] = jnp.full((pos, LANES), LOW, jnp.float32)
    for k in range(1, 4):
        stat[k] = jnp.zeros((pos, LANES), jnp.float32)

    def logits(src, count):
        turned = flip.at[:, 0:count]
        turned[...] = src[:, 0:FLIP].T
        z = jnp.dot(h_ref[:, 0:FLIP], turned[...], preferred_element_type=jnp.float32)
        z += lax.dot_general(h_ref[:, FLIP:], src[:, FLIP:], (((1,), (1,)), ((), ())),
                             preferred_element_type=jnp.float32)
        return [z[:, c:c + LANES] for c in range(0, count, LANES)]

    def fold(tiles, start):
        m_old = stat[0]
        m_new = tree(jnp.maximum, [m_old] + tiles)
        scale = jnp.exp(m_old - m_new)
        parts = [jnp.exp(t - m_new) for t in tiles]
        stat[0] = m_new
        stat[1] = tree(jnp.add, [stat[1] * scale] + parts)
        stat[2] = tree(jnp.add, [stat[2] * scale] + [e * t for e, t in zip(parts, tiles)])
        stat[3] = tree(jnp.add, [stat[3]] + [jnp.where(ids_rel == start + j * LANES, t, 0.0)
                                             for j, t in enumerate(tiles)])

    first.wait()
    fold(logits(odd, lead), 0)
    fetch(0).wait()
    for j, t in enumerate(logits(buf.at[0], BLOCK)):
        z_ref[j] = t

    def step(i, _):
        fetch(i).wait()
        nxt = i + DEPTH - 1

        @pl.when(nxt < steps)
        def _():
            fetch(nxt).start()

        tiles = logits(buf.at[lax.rem(i, DEPTH)], BLOCK)
        fold([z_ref[j] for j in range(BLOCK // LANES)], lead + (i - 1) * BLOCK)
        for j, t in enumerate(tiles):
            z_ref[j] = t
        return 0

    lax.fori_loop(1, steps, step, 0)
    fold([z_ref[j] for j in range(BLOCK // LANES)], lead + (steps - 1) * BLOCK)

    m_t, s_t, a_t, p_t = stat[0].T, stat[1].T, stat[2].T, stat[3].T
    m = jnp.max(m_t, axis=0, keepdims=True)
    wgt = jnp.exp(m_t - m)
    for k, v in enumerate((m, jnp.sum(s_t * wgt, axis=0, keepdims=True),
                           jnp.sum(a_t * wgt, axis=0, keepdims=True), jnp.sum(p_t, axis=0, keepdims=True))):
        mine[k:k + 1, :pos] = v
    got[me] = mine[...]
    pl.semaphore_wait(barrier, n_dev - 1)

    def send(peer):
        return pltpu.make_async_remote_copy(
            src_ref=mine, dst_ref=got.at[me], send_sem=side_sem.at[0], recv_sem=recv_sem,
            device_id={"tp": peer}, device_id_type=MESH)

    for peer in farthest_first(me, n_dev):
        send(peer).start()
    others = got.at[pl.ds(0, n_dev - 1)]
    exchange = pltpu.make_async_remote_copy(
        src_ref=others, dst_ref=others, send_sem=side_sem.at[0], recv_sem=recv_sem,
        device_id={"tp": me}, device_id_type=MESH)
    exchange.wait_recv()
    all_m = [got[d, 0:1, :pos] for d in range(n_dev)]
    top = tree(jnp.maximum, all_m)
    wgt = [jnp.exp(v - top) for v in all_m]
    out_ref[0:1, :pos] = top
    out_ref[1:2, :pos] = tree(jnp.add, [got[d, 1:2, :pos] * wgt[d] for d in range(n_dev)])
    out_ref[2:3, :pos] = tree(jnp.add, [got[d, 2:3, :pos] * wgt[d] for d in range(n_dev)])
    out_ref[3:4, :pos] = tree(jnp.add, [got[d, 3:4, :pos] for d in range(n_dev)])
    exchange.wait_send()


def solution(mesh):
    n_dev = mesh.shape["tp"]

    def local_part(hidden, norm_w, embedding, draft_ids):
        _, pos, width = hidden.shape
        hbm = pl.BlockSpec(memory_space=pltpu.HBM)
        vmem = pl.BlockSpec(memory_space=pltpu.VMEM)
        out = pl.pallas_call(
            functools.partial(head_kernel, n_dev),
            out_shape=pltpu.VMEM((4, LANES), jnp.float32),
            in_specs=[hbm] * 4,
            out_specs=vmem,
            scratch_shapes=[
                pltpu.VMEM((1, pos, width), jnp.bfloat16),
                pltpu.VMEM((width // LANES, LANES), jnp.bfloat16),
                pltpu.VMEM((1, pos), jnp.int32),
                pltpu.VMEM((pos, width), jnp.bfloat16),
                pltpu.VMEM((embedding.shape[0] % BLOCK, width), jnp.bfloat16),
                pltpu.VMEM((DEPTH, BLOCK, width), jnp.bfloat16),
                pltpu.VMEM((FLIP, BLOCK), jnp.bfloat16),
                pltpu.VMEM((BLOCK // LANES, pos, LANES), jnp.float32),
                pltpu.VMEM((4, pos, LANES), jnp.float32),
                pltpu.VMEM((4, LANES), jnp.float32),
                pltpu.VMEM((n_dev, 4, LANES), jnp.float32),
                pltpu.SemaphoreType.DMA,
            ],
            compiler_params=pltpu.CompilerParams(
                collective_id=0, has_side_effects=True, vmem_limit_bytes=60 * 2**20),
            cost_estimate=pl.CostEstimate(flops=2 * pos * embedding.size, bytes_accessed=2 * embedding.size,
                                          transcendentals=pos * embedding.shape[0]),
            name="head",
        )(hidden, norm_w.reshape(width // LANES, LANES), draft_ids, embedding)
        top, total, weighted, picked = (out[k:k + 1, :pos] for k in range(4))
        log_norm = top + jnp.log(total)
        return picked - log_norm, log_norm - weighted / total

    return jax.shard_map(local_part, mesh=mesh,
                         in_specs=(P("dp", None, None), P(None), P("tp", None), P("dp", None)),
                         out_specs=(P("dp", None), P("dp", None)), check_vma=False)
```

```python
import functools
import jax
import jax.numpy as jnp
from jax import lax
from jax.experimental import pallas as pl
from jax.experimental.pallas import tpu as pltpu
from jax.sharding import PartitionSpec as P

EPS = 1e-6
LANES = 128
BLOCK = 384
FLIP = 1024
DEPTH = 8
LOW = -3.0e38
MESH = pl.DeviceIdType.MESH


def tree(op, values):
    while len(values) > 1:
        values = [op(*values[k:k + 2]) if k + 1 < len(values) else values[k] for k in range(0, len(values), 2)]
    return values[0]


def farthest_first(me, n_dev):
    if n_dev != 8:
        return [lax.rem(me + d, n_dev) for d in range(1, n_dev)]
    y, x, core = me // 4, (me // 2) % 2, me % 2
    flipped = [(1, 1, 0), (1, 1, 1), (1, 0, 0), (0, 1, 0), (1, 0, 1), (0, 1, 1), (0, 0, 1)]
    return [(1 - y if a else y) * 4 + (1 - x if b else x) * 2 + (1 - core if c else core) for a, b, c in flipped]


def head_kernel(n_dev, *refs):
    pl.run_scoped(functools.partial(head_body, n_dev, *refs),
                  pltpu.SemaphoreType.DMA((DEPTH,)), pltpu.SemaphoreType.DMA((4,)))


def head_body(n_dev, x_hbm, w_hbm, ids_hbm, e_hbm, out_ref,
              x_ref, w_ref, ids_ref, h_ref, odd, buf, flip, z_ref, stat, mine, got, recv_sem,
              ring_sem, side_sem):
    rows, width = e_hbm.shape
    pos = x_ref.shape[1]
    lead = odd.shape[0]
    steps = (rows - lead) // BLOCK
    me = lax.axis_index("tp")
    barrier = pltpu.get_barrier_semaphore()

    small = [pltpu.make_async_copy(s, d, side_sem.at[k])
             for k, (s, d) in enumerate(((x_hbm, x_ref), (w_hbm, w_ref), (ids_hbm, ids_ref)))]
    first = pltpu.make_async_copy(e_hbm.at[pl.ds(0, lead), :], odd, side_sem.at[3])

    def fetch(i):
        slot = lax.rem(i, DEPTH)
        return pltpu.make_async_copy(e_hbm.at[pl.ds(lead + i * BLOCK, BLOCK), :], buf.at[slot], ring_sem.at[slot])

    first.start()
    fetch(0).start()
    for c in small:
        c.start()

    def prime(i, _):
        fetch(i).start()
        return 0

    lax.fori_loop(1, DEPTH, prime, 0)
    for d in range(1, n_dev):
        pl.semaphore_signal(barrier, inc=1, device_id={"tp": lax.rem(me + d, n_dev)}, device_id_type=MESH)
    for c in small:
        c.wait()

    x = x_ref[0].astype(jnp.float32)
    r = lax.rsqrt(jnp.mean(x * x, axis=-1, keepdims=True) + EPS)
    gain = 1.0 + w_ref[...].astype(jnp.float32)
    for c in range(width // LANES):
        cols = slice(c * LANES, (c + 1) * LANES)
        h_ref[:, cols] = (x[:, cols] * r * gain[c:c + 1, :]).astype(jnp.bfloat16)

    sub = lax.broadcasted_iota(jnp.int32, (pos, pos), 0)
    lan = lax.broadcasted_iota(jnp.int32, (pos, pos), 1)
    ids_row = jnp.broadcast_to(ids_ref[...], (pos, pos)).astype(jnp.float32)
    ids_col = jnp.sum(jnp.where(sub == lan, ids_row, 0.0), axis=1, keepdims=True).astype(jnp.int32)
    ids_rel = ids_col - me * rows - lax.broadcasted_iota(jnp.int32, (pos, LANES), 1)

    stat[0] = jnp.full((pos, LANES), LOW, jnp.float32)
    for k in range(1, 4):
        stat[k] = jnp.zeros((pos, LANES), jnp.float32)

    def logits(src, count):
        turned = flip.at[:, 0:count]
        turned[...] = src[:, 0:FLIP].T
        z = jnp.dot(h_ref[:, 0:FLIP], turned[...], preferred_element_type=jnp.float32)
        z += lax.dot_general(h_ref[:, FLIP:], src[:, FLIP:], (((1,), (1,)), ((), ())),
                             preferred_element_type=jnp.float32)
        return [z[:, c:c + LANES] for c in range(0, count, LANES)]

    def fold(tiles, start):
        m_old = stat[0]
        m_new = tree(jnp.maximum, [m_old] + tiles)
        scale = jnp.exp(m_old - m_new)
        parts = [jnp.exp(t - m_new) for t in tiles]
        stat[0] = m_new
        stat[1] = tree(jnp.add, [stat[1] * scale] + parts)
        stat[2] = tree(jnp.add, [stat[2] * scale] + [e * t for e, t in zip(parts, tiles)])
        stat[3] = tree(jnp.add, [stat[3]] + [jnp.where(ids_rel == start + j * LANES, t, 0.0)
                                             for j, t in enumerate(tiles)])

    first.wait()
    fold(logits(odd, lead), 0)
    fetch(0).wait()
    for j, t in enumerate(logits(buf.at[0], BLOCK)):
        z_ref[j] = t

    def step(i, _):
        fetch(i).wait()
        nxt = i + DEPTH - 1

        @pl.when(nxt < steps)
        def _():
            fetch(nxt).start()

        tiles = logits(buf.at[lax.rem(i, DEPTH)], BLOCK)
        fold([z_ref[j] for j in range(BLOCK // LANES)], lead + (i - 1) * BLOCK)
        for j, t in enumerate(tiles):
            z_ref[j] = t
        return 0

    lax.fori_loop(1, steps, step, 0)
    pl.semaphore_wait(barrier, n_dev - 1)
    peers = farthest_first(me, n_dev)
    fold([z_ref[j] for j in range(BLOCK // LANES)], lead + (steps - 1) * BLOCK)

    m_t, p_t, s_t, a_t = stat[0].T, stat[3].T, stat[1].T, stat[2].T
    m = jnp.max(m_t, axis=0, keepdims=True)
    wgt = jnp.exp(m_t - m)
    for k, v in enumerate((m, jnp.sum(s_t * wgt, axis=0, keepdims=True),
                           jnp.sum(a_t * wgt, axis=0, keepdims=True), jnp.sum(p_t, axis=0, keepdims=True))):
        mine[k:k + 1, :pos] = v
    got[me] = mine[...]

    def send(peer):
        return pltpu.make_async_remote_copy(
            src_ref=mine, dst_ref=got.at[me], send_sem=side_sem.at[0], recv_sem=recv_sem,
            device_id={"tp": peer}, device_id_type=MESH)

    for peer in peers:
        send(peer).start()
    others = got.at[pl.ds(0, n_dev - 1)]
    exchange = pltpu.make_async_remote_copy(
        src_ref=others, dst_ref=others, send_sem=side_sem.at[0], recv_sem=recv_sem,
        device_id={"tp": me}, device_id_type=MESH)
    exchange.wait_recv()
    all_m = [got[d, 0:1, :pos] for d in range(n_dev)]
    top = tree(jnp.maximum, all_m)
    wgt = [jnp.exp(v - top) for v in all_m]
    out_ref[0:1, :pos] = top
    out_ref[1:2, :pos] = tree(jnp.add, [got[d, 1:2, :pos] * wgt[d] for d in range(n_dev)])
    out_ref[2:3, :pos] = tree(jnp.add, [got[d, 2:3, :pos] * wgt[d] for d in range(n_dev)])
    out_ref[3:4, :pos] = tree(jnp.add, [got[d, 3:4, :pos] for d in range(n_dev)])
    exchange.wait_send()


def solution(mesh):
    n_dev = mesh.shape["tp"]

    def local_part(hidden, norm_w, embedding, draft_ids):
        _, pos, width = hidden.shape
        hbm = pl.BlockSpec(memory_space=pltpu.HBM)
        vmem = pl.BlockSpec(memory_space=pltpu.VMEM)
        out = pl.pallas_call(
            functools.partial(head_kernel, n_dev),
            out_shape=pltpu.VMEM((4, LANES), jnp.float32),
            in_specs=[hbm] * 4,
            out_specs=vmem,
            scratch_shapes=[
                pltpu.VMEM((1, pos, width), jnp.bfloat16),
                pltpu.VMEM((width // LANES, LANES), jnp.bfloat16),
                pltpu.VMEM((1, pos), jnp.int32),
                pltpu.VMEM((pos, width), jnp.bfloat16),
                pltpu.VMEM((embedding.shape[0] % BLOCK, width), jnp.bfloat16),
                pltpu.VMEM((DEPTH, BLOCK, width), jnp.bfloat16),
                pltpu.VMEM((FLIP, BLOCK), jnp.bfloat16),
                pltpu.VMEM((BLOCK // LANES, pos, LANES), jnp.float32),
                pltpu.VMEM((4, pos, LANES), jnp.float32),
                pltpu.VMEM((4, LANES), jnp.float32),
                pltpu.VMEM((n_dev, 4, LANES), jnp.float32),
                pltpu.SemaphoreType.DMA,
            ],
            compiler_params=pltpu.CompilerParams(
                collective_id=0, has_side_effects=True, vmem_limit_bytes=60 * 2**20),
            cost_estimate=pl.CostEstimate(flops=2 * pos * embedding.size, bytes_accessed=2 * embedding.size,
                                          transcendentals=pos * embedding.shape[0]),
            name="head",
        )(hidden, norm_w.reshape(width // LANES, LANES), draft_ids, embedding)
        top, total, weighted, picked = (out[k:k + 1, :pos] for k in range(4))
        log_norm = top + jnp.log(total)
        return picked - log_norm, log_norm - weighted / total

    return jax.shard_map(local_part, mesh=mesh,
                         in_specs=(P("dp", None, None), P(None), P("tp", None), P("dp", None)),
                         out_specs=(P("dp", None), P("dp", None)), check_vma=False)
```

```python
import functools
import jax
import jax.numpy as jnp
from jax import lax
from jax.experimental import pallas as pl
from jax.experimental.pallas import tpu as pltpu
from jax.sharding import PartitionSpec as P

EPS = 1e-6
LANES = 128
BLOCK = 384
FLIP = 1024
DEPTH = 8
LOW = -3.0e38
MESH = pl.DeviceIdType.MESH


def tree(op, values):
    while len(values) > 1:
        values = [op(*values[k:k + 2]) if k + 1 < len(values) else values[k] for k in range(0, len(values), 2)]
    return values[0]


def farthest_first(me, n_dev):
    if n_dev != 8:
        return [lax.rem(me + d, n_dev) for d in range(1, n_dev)]
    y, x, core = me // 4, (me // 2) % 2, me % 2
    flipped = [(1, 1, 0), (1, 1, 1), (1, 0, 0), (0, 1, 0), (1, 0, 1), (0, 1, 1), (0, 0, 1)]
    return [(1 - y if a else y) * 4 + (1 - x if b else x) * 2 + (1 - core if c else core) for a, b, c in flipped]


def head_kernel(n_dev, *refs):
    pl.run_scoped(functools.partial(head_body, n_dev, *refs),
                  pltpu.SemaphoreType.DMA((DEPTH,)), pltpu.SemaphoreType.DMA((4,)))


def head_body(n_dev, x_hbm, w_hbm, ids_hbm, e_hbm, out_ref,
              x_ref, w_ref, ids_ref, h_ref, odd, buf, flip, z_ref, stat, mine, got, recv_sem,
              ring_sem, side_sem):
    rows, width = e_hbm.shape
    pos = x_ref.shape[1]
    lead = odd.shape[0]
    steps = (rows - lead) // BLOCK
    me = lax.axis_index("tp")
    barrier = pltpu.get_barrier_semaphore()

    small = [pltpu.make_async_copy(s, d, side_sem.at[k])
             for k, (s, d) in enumerate(((x_hbm, x_ref), (w_hbm, w_ref), (ids_hbm, ids_ref)))]
    first = pltpu.make_async_copy(e_hbm.at[pl.ds(0, lead), :], odd, side_sem.at[3])

    def fetch(i):
        slot = lax.rem(i, DEPTH)
        return pltpu.make_async_copy(e_hbm.at[pl.ds(lead + i * BLOCK, BLOCK), :], buf.at[slot], ring_sem.at[slot])

    first.start()
    fetch(0).start()
    for c in small:
        c.start()

    def prime(i, _):
        fetch(i).start()
        return 0

    lax.fori_loop(1, DEPTH, prime, 0)
    for d in range(1, n_dev):
        pl.semaphore_signal(barrier, inc=1, device_id={"tp": lax.rem(me + d, n_dev)}, device_id_type=MESH)
    for c in small:
        c.wait()

    x = x_ref[0].astype(jnp.float32)
    r = lax.rsqrt(jnp.mean(x * x, axis=-1, keepdims=True) + EPS)
    gain = 1.0 + w_ref[...].astype(jnp.float32)
    for c in range(width // LANES):
        cols = slice(c * LANES, (c + 1) * LANES)
        h_ref[:, cols] = (x[:, cols] * r * gain[c:c + 1, :]).astype(jnp.bfloat16)

    sub = lax.broadcasted_iota(jnp.int32, (pos, pos), 0)
    lan = lax.broadcasted_iota(jnp.int32, (pos, pos), 1)
    ids_row = jnp.broadcast_to(ids_ref[...], (pos, pos)).astype(jnp.float32)
    ids_col = jnp.sum(jnp.where(sub == lan, ids_row, 0.0), axis=1, keepdims=True).astype(jnp.int32)
    ids_rel = ids_col - me * rows - lax.broadcasted_iota(jnp.int32, (pos, LANES), 1)

    stat[0] = jnp.full((pos, LANES), LOW, jnp.float32)
    for k in range(1, 4):
        stat[k] = jnp.zeros((pos, LANES), jnp.float32)

    def logits(src, count):
        turned = flip.at[:, 0:count]
        turned[...] = src[:, 0:FLIP].T
        z = jnp.dot(h_ref[:, 0:FLIP], turned[...], preferred_element_type=jnp.float32)
        z += lax.dot_general(h_ref[:, FLIP:], src[:, FLIP:], (((1,), (1,)), ((), ())),
                             preferred_element_type=jnp.float32)
        return [z[:, c:c + LANES] for c in range(0, count, LANES)]

    def fold(tiles, start):
        m_old = stat[0]
        m_new = tree(jnp.maximum, [m_old] + tiles)
        scale = jnp.exp(m_old - m_new)
        parts = [jnp.exp(t - m_new) for t in tiles]
        stat[0] = m_new
        stat[1] = tree(jnp.add, [stat[1] * scale] + parts)
        stat[2] = tree(jnp.add, [stat[2] * scale] + [e * t for e, t in zip(parts, tiles)])
        stat[3] = tree(jnp.add, [stat[3]] + [jnp.where(ids_rel == start + j * LANES, t, 0.0)
                                             for j, t in enumerate(tiles)])

    first.wait()
    fold(logits(odd, lead), 0)
    fetch(0).wait()
    for j, t in enumerate(logits(buf.at[0], BLOCK)):
        z_ref[j] = t

    def step(i, _):
        fetch(i).wait()
        nxt = i + DEPTH - 1

        @pl.when(nxt < steps)
        def _():
            fetch(nxt).start()

        tiles = logits(buf.at[lax.rem(i, DEPTH)], BLOCK)
        fold([z_ref[j] for j in range(BLOCK // LANES)], lead + (i - 1) * BLOCK)
        for j, t in enumerate(tiles):
            z_ref[j] = t
        return 0

    lax.fori_loop(1, steps - 1, step, 0)
    pl.semaphore_wait(barrier, n_dev - 1)
    peers = farthest_first(me, n_dev)
    fetch(steps - 1).wait()
    tiles = logits(buf.at[(steps - 1) % DEPTH], BLOCK)
    fold([z_ref[j] for j in range(BLOCK // LANES)], lead + (steps - 2) * BLOCK)
    fold(tiles, lead + (steps - 1) * BLOCK)

    m_t, p_t, s_t, a_t = stat[0].T, stat[3].T, stat[1].T, stat[2].T
    m = jnp.max(m_t, axis=0, keepdims=True)
    wgt = jnp.exp(m_t - m)
    for k, v in enumerate((m, jnp.sum(s_t * wgt, axis=0, keepdims=True),
                           jnp.sum(a_t * wgt, axis=0, keepdims=True), jnp.sum(p_t, axis=0, keepdims=True))):
        mine[k:k + 1, :pos] = v
    got[me] = mine[...]

    def send(peer):
        return pltpu.make_async_remote_copy(
            src_ref=mine, dst_ref=got.at[me], send_sem=side_sem.at[0], recv_sem=recv_sem,
            device_id={"tp": peer}, device_id_type=MESH)

    for peer in peers:
        send(peer).start()
    others = got.at[pl.ds(0, n_dev - 1)]
    exchange = pltpu.make_async_remote_copy(
        src_ref=others, dst_ref=others, send_sem=side_sem.at[0], recv_sem=recv_sem,
        device_id={"tp": me}, device_id_type=MESH)
    exchange.wait_recv()
    all_m = [got[d, 0:1, :pos] for d in range(n_dev)]
    top = tree(jnp.maximum, all_m)
    wgt = [jnp.exp(v - top) for v in all_m]
    out_ref[0:1, :pos] = top
    out_ref[1:2, :pos] = tree(jnp.add, [got[d, 1:2, :pos] * wgt[d] for d in range(n_dev)])
    out_ref[2:3, :pos] = tree(jnp.add, [got[d, 2:3, :pos] * wgt[d] for d in range(n_dev)])
    out_ref[3:4, :pos] = tree(jnp.add, [got[d, 3:4, :pos] for d in range(n_dev)])
    exchange.wait_send()


def solution(mesh):
    n_dev = mesh.shape["tp"]

    def local_part(hidden, norm_w, embedding, draft_ids):
        _, pos, width = hidden.shape
        hbm = pl.BlockSpec(memory_space=pltpu.HBM)
        vmem = pl.BlockSpec(memory_space=pltpu.VMEM)
        out = pl.pallas_call(
            functools.partial(head_kernel, n_dev),
            out_shape=pltpu.VMEM((4, LANES), jnp.float32),
            in_specs=[hbm] * 4,
            out_specs=vmem,
            scratch_shapes=[
                pltpu.VMEM((1, pos, width), jnp.bfloat16),
                pltpu.VMEM((width // LANES, LANES), jnp.bfloat16),
                pltpu.VMEM((1, pos), jnp.int32),
                pltpu.VMEM((pos, width), jnp.bfloat16),
                pltpu.VMEM((embedding.shape[0] % BLOCK, width), jnp.bfloat16),
                pltpu.VMEM((DEPTH, BLOCK, width), jnp.bfloat16),
                pltpu.VMEM((FLIP, BLOCK), jnp.bfloat16),
                pltpu.VMEM((BLOCK // LANES, pos, LANES), jnp.float32),
                pltpu.VMEM((4, pos, LANES), jnp.float32),
                pltpu.VMEM((4, LANES), jnp.float32),
                pltpu.VMEM((n_dev, 4, LANES), jnp.float32),
                pltpu.SemaphoreType.DMA,
            ],
            compiler_params=pltpu.CompilerParams(
                collective_id=0, has_side_effects=True, vmem_limit_bytes=60 * 2**20),
            cost_estimate=pl.CostEstimate(flops=2 * pos * embedding.size, bytes_accessed=2 * embedding.size,
                                          transcendentals=pos * embedding.shape[0]),
            name="head",
        )(hidden, norm_w.reshape(width // LANES, LANES), draft_ids, embedding)
        top, total, weighted, picked = (out[k:k + 1, :pos] for k in range(4))
        log_norm = top + jnp.log(total)
        return picked - log_norm, log_norm - weighted / total

    return jax.shard_map(local_part, mesh=mesh,
                         in_specs=(P("dp", None, None), P(None), P("tp", None), P("dp", None)),
                         out_specs=(P("dp", None), P("dp", None)), check_vma=False)
```

```python
import functools
import jax
import jax.numpy as jnp
from jax import lax
from jax.experimental import pallas as pl
from jax.experimental.pallas import tpu as pltpu
from jax.sharding import PartitionSpec as P

EPS = 1e-6
LANES = 128
BLOCK = 384
FLIP = 1024
DEPTH = 8
LOW = -3.0e38
MESH = pl.DeviceIdType.MESH


def tree(op, values):
    while len(values) > 1:
        values = [op(*values[k:k + 2]) if k + 1 < len(values) else values[k] for k in range(0, len(values), 2)]
    return values[0]


def farthest_first(me, n_dev):
    if n_dev != 8:
        return [lax.rem(me + d, n_dev) for d in range(1, n_dev)]
    y, x, core = me // 4, (me // 2) % 2, me % 2
    flipped = [(1, 1, 0), (0, 0, 1), (1, 0, 0), (0, 1, 0), (1, 0, 1), (0, 1, 1), (1, 1, 1)]
    return [(1 - y if a else y) * 4 + (1 - x if b else x) * 2 + (1 - core if c else core) for a, b, c in flipped]


def head_kernel(n_dev, *refs):
    pl.run_scoped(functools.partial(head_body, n_dev, *refs),
                  pltpu.SemaphoreType.DMA((DEPTH,)), pltpu.SemaphoreType.DMA((4,)))


def head_body(n_dev, x_hbm, w_hbm, ids_hbm, e_hbm, out_ref,
              x_ref, w_ref, ids_ref, h_ref, odd, buf, flip, z_ref, stat, mine, got, recv_sem,
              ring_sem, side_sem):
    rows, width = e_hbm.shape
    pos = x_ref.shape[1]
    lead = odd.shape[0]
    steps = (rows - lead) // BLOCK
    me = lax.axis_index("tp")
    barrier = pltpu.get_barrier_semaphore()

    small = [pltpu.make_async_copy(s, d, side_sem.at[k])
             for k, (s, d) in enumerate(((x_hbm, x_ref), (w_hbm, w_ref), (ids_hbm, ids_ref)))]
    first = pltpu.make_async_copy(e_hbm.at[pl.ds(0, lead), :], odd, side_sem.at[3])

    def fetch(i):
        slot = lax.rem(i, DEPTH)
        return pltpu.make_async_copy(e_hbm.at[pl.ds(lead + i * BLOCK, BLOCK), :], buf.at[slot], ring_sem.at[slot])

    first.start()
    fetch(0).start()
    for c in small:
        c.start()

    def prime(i, _):
        fetch(i).start()
        return 0

    lax.fori_loop(1, DEPTH, prime, 0)
    for d in range(1, n_dev):
        pl.semaphore_signal(barrier, inc=1, device_id={"tp": lax.rem(me + d, n_dev)}, device_id_type=MESH)
    for c in small:
        c.wait()

    x = x_ref[0].astype(jnp.float32)
    r = lax.rsqrt(jnp.mean(x * x, axis=-1, keepdims=True) + EPS)
    gain = 1.0 + w_ref[...].astype(jnp.float32)
    for c in range(width // LANES):
        cols = slice(c * LANES, (c + 1) * LANES)
        h_ref[:, cols] = (x[:, cols] * r * gain[c:c + 1, :]).astype(jnp.bfloat16)

    sub = lax.broadcasted_iota(jnp.int32, (pos, pos), 0)
    lan = lax.broadcasted_iota(jnp.int32, (pos, pos), 1)
    ids_row = jnp.broadcast_to(ids_ref[...], (pos, pos)).astype(jnp.float32)
    ids_col = jnp.sum(jnp.where(sub == lan, ids_row, 0.0), axis=1, keepdims=True).astype(jnp.int32)
    ids_rel = ids_col - me * rows - lax.broadcasted_iota(jnp.int32, (pos, LANES), 1)

    stat[0] = jnp.full((pos, LANES), LOW, jnp.float32)
    for k in range(1, 4):
        stat[k] = jnp.zeros((pos, LANES), jnp.float32)

    def logits(src, count):
        turned = flip.at[:, 0:count]
        turned[...] = src[:, 0:FLIP].T
        z = jnp.dot(h_ref[:, 0:FLIP], turned[...], preferred_element_type=jnp.float32)
        z += lax.dot_general(h_ref[:, FLIP:], src[:, FLIP:], (((1,), (1,)), ((), ())),
                             preferred_element_type=jnp.float32)
        return [z[:, c:c + LANES] for c in range(0, count, LANES)]

    def fold(tiles, start):
        m_old = stat[0]
        m_new = tree(jnp.maximum, [m_old] + tiles)
        scale = jnp.exp(m_old - m_new)
        parts = [jnp.exp(t - m_new) for t in tiles]
        stat[0] = m_new
        stat[1] = tree(jnp.add, [stat[1] * scale] + parts)
        stat[2] = tree(jnp.add, [stat[2] * scale] + [e * t for e, t in zip(parts, tiles)])
        stat[3] = tree(jnp.add, [stat[3]] + [jnp.where(ids_rel == start + j * LANES, t, 0.0)
                                             for j, t in enumerate(tiles)])

    first.wait()
    fold(logits(odd, lead), 0)
    fetch(0).wait()
    for j, t in enumerate(logits(buf.at[0], BLOCK)):
        z_ref[j] = t

    def step(i, _):
        fetch(i).wait()
        nxt = i + DEPTH - 1

        @pl.when(nxt < steps)
        def _():
            fetch(nxt).start()

        tiles = logits(buf.at[lax.rem(i, DEPTH)], BLOCK)
        fold([z_ref[j] for j in range(BLOCK // LANES)], lead + (i - 1) * BLOCK)
        for j, t in enumerate(tiles):
            z_ref[j] = t
        return 0

    lax.fori_loop(1, steps - 1, step, 0)
    pl.semaphore_wait(barrier, n_dev - 1)
    peers = farthest_first(me, n_dev)
    fetch(steps - 1).wait()
    tiles = logits(buf.at[(steps - 1) % DEPTH], BLOCK)
    fold([z_ref[j] for j in range(BLOCK // LANES)], lead + (steps - 2) * BLOCK)
    fold(tiles, lead + (steps - 1) * BLOCK)

    m_t, p_t, s_t, a_t = stat[0].T, stat[3].T, stat[1].T, stat[2].T
    m = jnp.max(m_t, axis=0, keepdims=True)
    wgt = jnp.exp(m_t - m)
    for k, v in enumerate((m, jnp.sum(s_t * wgt, axis=0, keepdims=True),
                           jnp.sum(a_t * wgt, axis=0, keepdims=True), jnp.sum(p_t, axis=0, keepdims=True))):
        mine[k:k + 1, :pos] = v
    got[me] = mine[...]

    def send(peer):
        return pltpu.make_async_remote_copy(
            src_ref=mine, dst_ref=got.at[me], send_sem=side_sem.at[0], recv_sem=recv_sem,
            device_id={"tp": peer}, device_id_type=MESH)

    for peer in peers:
        send(peer).start()
    others = got.at[pl.ds(0, n_dev - 1)]
    exchange = pltpu.make_async_remote_copy(
        src_ref=others, dst_ref=others, send_sem=side_sem.at[0], recv_sem=recv_sem,
        device_id={"tp": me}, device_id_type=MESH)
    exchange.wait_recv()
    all_m = [got[d, 0:1, :pos] for d in range(n_dev)]
    top = tree(jnp.maximum, all_m)
    wgt = [jnp.exp(v - top) for v in all_m]
    out_ref[0:1, :pos] = top
    out_ref[1:2, :pos] = tree(jnp.add, [got[d, 1:2, :pos] * wgt[d] for d in range(n_dev)])
    out_ref[2:3, :pos] = tree(jnp.add, [got[d, 2:3, :pos] * wgt[d] for d in range(n_dev)])
    out_ref[3:4, :pos] = tree(jnp.add, [got[d, 3:4, :pos] for d in range(n_dev)])
    exchange.wait_send()


def solution(mesh):
    n_dev = mesh.shape["tp"]

    def local_part(hidden, norm_w, embedding, draft_ids):
        _, pos, width = hidden.shape
        hbm = pl.BlockSpec(memory_space=pltpu.HBM)
        vmem = pl.BlockSpec(memory_space=pltpu.VMEM)
        out = pl.pallas_call(
            functools.partial(head_kernel, n_dev),
            out_shape=pltpu.VMEM((4, LANES), jnp.float32),
            in_specs=[hbm] * 4,
            out_specs=vmem,
            scratch_shapes=[
                pltpu.VMEM((1, pos, width), jnp.bfloat16),
                pltpu.VMEM((width // LANES, LANES), jnp.bfloat16),
                pltpu.VMEM((1, pos), jnp.int32),
                pltpu.VMEM((pos, width), jnp.bfloat16),
                pltpu.VMEM((embedding.shape[0] % BLOCK, width), jnp.bfloat16),
                pltpu.VMEM((DEPTH, BLOCK, width), jnp.bfloat16),
                pltpu.VMEM((FLIP, BLOCK), jnp.bfloat16),
                pltpu.VMEM((BLOCK // LANES, pos, LANES), jnp.float32),
                pltpu.VMEM((4, pos, LANES), jnp.float32),
                pltpu.VMEM((4, LANES), jnp.float32),
                pltpu.VMEM((n_dev, 4, LANES), jnp.float32),
                pltpu.SemaphoreType.DMA,
            ],
            compiler_params=pltpu.CompilerParams(
                collective_id=0, has_side_effects=True, vmem_limit_bytes=60 * 2**20),
            cost_estimate=pl.CostEstimate(flops=2 * pos * embedding.size, bytes_accessed=2 * embedding.size,
                                          transcendentals=pos * embedding.shape[0]),
            name="head",
        )(hidden, norm_w.reshape(width // LANES, LANES), draft_ids, embedding)
        top, total, weighted, picked = (out[k:k + 1, :pos] for k in range(4))
        log_norm = top + jnp.log(total)
        return picked - log_norm, log_norm - weighted / total

    return jax.shard_map(local_part, mesh=mesh,
                         in_specs=(P("dp", None, None), P(None), P("tp", None), P("dp", None)),
                         out_specs=(P("dp", None), P("dp", None)), check_vma=False)
```
